32 devices in a mesh: bvec: 4 (over y, x), row: 2 (over core), col: 4 (over z).
Axes of the slice: x: 2, y: 2, z: 4, core: 2. Of those that a mesh axis runs over, the one named last changes fastest.
Arguments:
- m_matrices: float32 [4, 2, 2048, 2048], P('bvec', None, 'row', 'col'), may hold values from -2 to 2, as said below
- bvec_index: int32 [4], replicated, may hold values from 0 to 5
- weight_table: float32 [6], replicated, may hold values from 0.25 to 2
- grad_prev: float32 [2048, 2048], P('row', 'col'), may hold values from -4 to 4, as said below
- dir_prev: float32 [2048, 2048], P('row', 'col'), may hold values from -4 to 4, as said below
Outputs:
- spread: float32 [], replicated
- trial_spread: float32 [], replicated
- gradient: float32 [2048, 2048], P('row', 'col')
- direction: float32 [2048, 2048], P('row', 'col')
- trial_diag: float32 [4, 2, 2048], replicated
The draws below stay inside these ranges and needn't reach their ends.
Inputs may be any that keep to these rules, and one draw needn't show every extreme that they name: Each matrix m_matrices[b, p] is symmetric. grad_prev is antisymmetric. dir_prev is antisymmetric.
All inputs are finite; a program needn't handle non-finite values.
Results may differ from the reference program's by a relative error of at most 0.0003.
Values sent between devices are 32-bit elements; how exact they have to be, the bound alone decides.
No kernel may reach another device: no remote copies, remote signals or barrier semaphores. Data moves between devices by JAX's collectives and lax.ppermute only.
A program may use at most 128 MiB of HBM per device.

```python
import math
import jax
import jax.numpy as jnp
from jax import lax

N = 2048
NTAB = 6
TAYLOR = 8
NB = 4


def draw_m_matrices(key, part):
    subkeys = jax.random.split(jax.random.fold_in(key, 101), 4)
    gaussian = jax.random.normal(subkeys[0], (NB, 2, N, N), jnp.float32)
    noise_scale = 0.25
    radius = jax.random.uniform(subkeys[1], (NB, N), jnp.float32, 0.3, 0.95)
    angles = jax.random.uniform(subkeys[2], (NB, N), jnp.float32, -math.pi, math.pi)
    symmetric = (gaussian + jnp.swapaxes(gaussian, 2, 3)) * (noise_scale / math.sqrt(2.0))
    identity = jnp.eye(N, dtype=jnp.float32)
    diag_parts = jnp.stack([radius * jnp.cos(angles), radius * jnp.sin(angles)], axis=1)
    matrix = symmetric * (1.0 - identity) + diag_parts[:, :, :, None] * identity
    return jnp.clip(matrix, -2.0, 2.0)


def antisymmetric(key, noise_scale):
    gaussian = jax.random.normal(key, (N, N), jnp.float32)
    factor = noise_scale
    return jnp.clip((gaussian - gaussian.T) * (factor / math.sqrt(2.0)), -4.0, 4.0)


def draw_grad_prev(key, part):
    return antisymmetric(jax.random.fold_in(key, 7), 0.6)


def draw_dir_prev(key, part):
    return antisymmetric(jax.random.fold_in(key, 13), 0.6)


def plant(array, rng, smallest, top_value):
    spot = [jax.random.randint(jax.random.fold_in(rng, axis), (), 0, length) for axis, length in enumerate(array.shape)]
    longest = array.shape.index(max(array.shape))
    neighbour = spot[:longest] + [(spot[longest] + 1) % array.shape[longest]] + spot[longest + 1:]
    return array.at[tuple(spot)].set(smallest).at[tuple(neighbour)].set(top_value)


def setup_inputs(seed: int = 0) -> dict:
    seeds = jax.random.split(jax.random.key(seed), 6)
    return {
        "m_matrices": draw_m_matrices(jax.random.fold_in(seeds[5], 71), 0),
        "bvec_index": plant(jax.random.randint(seeds[1], (NB,), 0, NTAB), jax.random.fold_in(seeds[1], 1), 0, NTAB - 1).astype(jnp.int32),
        "weight_table": jnp.clip(jnp.exp(jax.random.uniform(seeds[2], (NTAB,), jnp.float32, math.log(0.25), math.log(2.0))), 0.25, 2.0),
        "grad_prev": draw_grad_prev(jax.random.fold_in(seeds[5], 71), 0),
        "dir_prev": draw_dir_prev(jax.random.fold_in(seeds[5], 71), 0),
    }


def product(left, right):
    return jnp.dot(left, right, precision=lax.Precision.HIGHEST, preferred_element_type=jnp.float32)

def reference(m_matrices, bvec_index, weight_table, grad_prev, dir_prev):
    table_slots = jnp.arange(weight_table.shape[0], dtype=jnp.int32)
    weight = lax.optimization_barrier(jnp.sum(jnp.where(table_slots[None, :] == bvec_index[:, None], weight_table[None, :], 0.0), axis=1))
    re_diag = jnp.diagonal(m_matrices[:, 0], axis1=1, axis2=2)
    im_diag = jnp.diagonal(m_matrices[:, 1], axis1=1, axis2=2)
    spread = jnp.sum(weight[:, None] * (1.0 - re_diag ** 2 - im_diag ** 2)) / N
    gradient = jnp.zeros((N, N), jnp.float32)
    for bvec in range(NB):
        real_term = m_matrices[bvec, 0] * (re_diag[bvec][:, None] - re_diag[bvec][None, :])
        imag_term = m_matrices[bvec, 1] * (im_diag[bvec][:, None] - im_diag[bvec][None, :])
        gradient = gradient + 2.0 * weight[bvec] * (real_term + imag_term)
    beta_factor = jnp.sum(gradient * gradient) / (1.0 + jnp.sum(grad_prev * grad_prev))
    direction = beta_factor * dir_prev - gradient
    trial_generator = 1.75 * direction / jnp.sqrt(1.0 + jnp.sum(direction * direction) / N)
    identity = jnp.eye(N, dtype=jnp.float32)
    horner = identity + trial_generator / TAYLOR
    for degree in range(TAYLOR - 1, 0, -1):
        horner = identity + product(horner, trial_generator) / degree
    expmap = horner
    entries = []
    for bvec in range(NB):
        parts = []
        for index in range(2):
            rotated = product(m_matrices[bvec, index], expmap)
            parts.append(lax.optimization_barrier(jnp.sum(expmap * rotated, axis=0)))
        entries.append(jnp.stack(parts, axis=0))
    trial_diag = jnp.stack(entries, axis=0)
    trial_spread = jnp.sum(weight[:, None] * (1.0 - trial_diag[:, 0] ** 2 - trial_diag[:, 1] ** 2)) / N
    return (spread, trial_spread, gradient, direction, trial_diag)
```

```python
import jax
import jax.numpy as jnp
from jax import lax
from jax.experimental import pallas as pl
from jax.experimental.pallas import tpu as pltpu
from jax.sharding import PartitionSpec as P


TAYLOR = 8
STEP_SCALE = 1.75
HIGHEST = lax.Precision.HIGHEST
AXES = ("bvec", "row", "col")
ANY = pl.BlockSpec(memory_space=pl.ANY)
SMEM = pl.BlockSpec(memory_space=pltpu.SMEM)
VMEM = pl.BlockSpec(memory_space=pltpu.VMEM)
VMEM_LIMIT = 62 * 1024 * 1024


def split_bf16(x):
    high = x.astype(jnp.bfloat16)
    low = (x - high.astype(jnp.float32)).astype(jnp.bfloat16)
    return high, low


def dot(a, b):
    return jnp.dot(a, b, preferred_element_type=jnp.float32)


def above(n):
    return lax.broadcasted_iota(jnp.int32, (n, n), 1) > lax.broadcasted_iota(jnp.int32, (n, n), 0)


def pack_block(part, o, value, low_half):
    n = value.shape[0] // 2

    def put(i, rows):
        part[i // 2, i % 2 * n:(i % 2 + 1) * n, :] = rows

    if o == 0:
        mixed = jnp.where(above(n), value[:n, :n], value[n:, n:])
        put(0, jnp.concatenate([mixed, value[:n, n:]], axis=1))
    elif o == 4:
        put(7, jnp.where(low_half, value[:n, :], value[:, n:].T))
    else:
        put(2 * o - 1, value[:n])
        put(2 * o, value[n:])


def unpack_diagonal(rows):
    n = rows.shape[0]
    mixed, corner = rows[:, :n], rows[:, n:]
    upper = jnp.where(above(n), mixed, 0.0)
    below = lax.broadcasted_iota(jnp.int32, (n, n), 1) < lax.broadcasted_iota(jnp.int32, (n, n), 0)
    lower = jnp.where(below, mixed, 0.0)
    return upper - upper.T, corner, -corner.T, lower - lower.T


def term_kernel(ids, weight, diags, own, other, o0, o1, o2, o3, chosen, mre, mim, part, sem, out_sem, chosen_sem):
    b, r, z = ids[0], ids[1], ids[2]
    size = mre.shape[-1]
    per_core = own.shape[1] // size
    blocks = 2 * per_core
    kept = mre.shape[0]
    per_chip = own.shape[2] // size
    groups = blocks // per_chip
    j = z * per_chip + r
    lanes = pl.ds(pl.multiple_of(r * size, size), size)
    for o in range(kept):
        block = lax.rem(j + o, blocks)
        rows = pl.ds(pl.multiple_of(lax.rem(block, per_core) * size, size), size)
        mine = lax.div(block, per_core) == r
        for ref, cond in ((own, mine), (other, jnp.logical_not(mine))):
            @pl.when(cond)
            def _(ref=ref, o=o, rows=rows):
                pltpu.make_async_copy(ref.at[0, rows, lanes], mre.at[o], sem.at[0, o]).start()
                pltpu.make_async_copy(ref.at[1, rows, lanes], mim.at[o], sem.at[1, o]).start()

    def piece(block, p):
        slot = lax.rem(z - lax.div(block, per_chip) + groups, groups)
        half = lax.rem(block, per_chip)
        row = diags[slot, pl.ds(p, 1), :]
        return jnp.where(half == 0, row[:, :size], row[:, size:])

    factor = 2.0 * weight[0]
    re_own, im_own = piece(j, 0), piece(j, 1)
    low_half = j < blocks // 2
    copies = []
    for o in range(kept):
        block = lax.rem(j + o, blocks)
        re_rows = jnp.broadcast_to(piece(block, 0), (size, size)).T
        im_rows = jnp.broadcast_to(piece(block, 1), (size, size)).T
        pltpu.make_async_copy(own.at[0, pl.ds(0, size), pl.ds(0, size)], mre.at[o], sem.at[0, o]).wait()
        pltpu.make_async_copy(own.at[0, pl.ds(0, size), pl.ds(0, size)], mim.at[o], sem.at[1, o]).wait()
        kept_copies = [pltpu.make_async_copy(buf.at[o], chosen.at[p, o], chosen_sem.at[p, o]) for p, buf in enumerate((mre, mim))]
        for copy in kept_copies:
            copy.start()
        copies += kept_copies
        value = factor * (mre[o] * (re_rows - re_own) + mim[o] * (im_rows - im_own))
        pack_block(part, o, value, low_half)
    for k, out in enumerate((o0, o1, o2, o3)):
        copy = pltpu.make_async_copy(part.at[jnp.bitwise_xor(b, k)], out, out_sem.at[k])
        copy.start()
        copies.append(copy)
    for copy in copies:
        copy.wait()


def quarter_kernel(ids, own, other, out, half, buf, sem):
    r, z, h = ids[1], ids[2], ids[4]
    size = buf.shape[2]
    per_core = own.shape[0] // size
    blocks = 2 * per_core
    per_chip = own.shape[1] // size
    j = z * per_chip + r
    lanes = pl.ds(pl.multiple_of(r * size, size), size)
    for o in range(5):
        block = lax.rem(j + o, blocks)
        rows = pl.ds(pl.multiple_of(lax.rem(block, per_core) * size, size), size)
        mine = lax.div(block, per_core) == r
        for ref, cond in ((own, mine), (other, jnp.logical_not(mine))):
            @pl.when(cond)
            def _(ref=ref, rows=rows, o=o):
                pltpu.make_async_copy(ref.at[rows, lanes], buf.at[o], sem.at[o]).start()
    for o in range(5):
        pltpu.make_async_copy(own.at[pl.ds(0, size), pl.ds(0, size)], buf.at[o], sem.at[o]).wait()
        pack_block(out, o, buf[o], j < blocks // 2)
    half[...] = jnp.where(h == 0, out[0:2], out[2:4])


def group_copies(ids, ins, dst, sem, place):
    r, z = ids[1], ids[2]
    groups = len(ins) // 2
    quarter = ins[0].shape[1]
    out = []
    for i, ref in enumerate(ins):
        s, c = i % groups, i // groups
        j = lax.rem(z - s + groups, groups) * 2 + (r if c == 0 else 1 - r)
        for k in range(4):
            rows = pl.ds(pl.multiple_of(place(s, k) * quarter, quarter), quarter)
            out.append(pltpu.make_async_copy(ref.at[k], dst.at[j, rows], sem.at[i]))
    return out


def terms_place(ids):
    return lambda s, k: jnp.bitwise_xor(ids[0], k)


def shared_place(ids):
    h = ids[4]
    return lambda s, k: k if s == 0 else (2 * h + k if k < 2 else 2 * (1 - h) + k - 2)


def solve_kernel(ids, prev_square, *refs):
    groups = (len(refs) - 9) // 4
    g_in, d_in = refs[:2 * groups], refs[2 * groups:4 * groups]
    beta_out, exp_out, pg, pd, ahi, alo, hhi, hlo, sem = refs[4 * groups:]
    own_block = ids[3]
    order = ahi.shape[0]
    blocks, _, size = pg.shape

    g_copies = group_copies(ids, g_in, pg, sem.at[0], terms_place(ids))
    d_copies = group_copies(ids, d_in, pd, sem.at[1], shared_place(ids))
    for c in g_copies + d_copies:
        c.start()
    strip = size // 2

    def fold(x):
        return jnp.sum(x.reshape(-1, 8, size), axis=0)

    quarter = g_in[0].shape[1]

    def arrive(which, i):
        for k in range(4):
            at = pl.ds(k * quarter, quarter)
            pltpu.make_async_copy(g_in[0].at[k], pg.at[0, at], sem.at[which, i]).wait()
        core = lax.div(i, groups)
        column = lax.rem(ids[2] - lax.rem(i, groups) + groups, groups) * 2
        return column + jnp.where(core == 0, ids[1], 1 - ids[1])

    def norm_body(i, acc):
        jj = arrive(0, i)
        for t in range(0, pg.shape[1], size):
            v = pg[jj, t:t + size, :]
            acc = acc + fold(v * v)
        return acc

    zero = jnp.zeros((8, size), jnp.float32)
    beta = 2.0 * jnp.sum(lax.fori_loop(0, blocks, norm_body, zero)) / (1.0 + prev_square[0])
    beta_out[...] = jnp.full(beta_out.shape, beta, jnp.float32)

    def store(row, col, v):
        high, low = split_bf16(v)
        rows = pl.ds(pl.multiple_of(row, strip), v.shape[0])
        cols = pl.ds(pl.multiple_of(col, strip), v.shape[1])
        ahi[rows, cols] = high
        alo[rows, cols] = low

    def dir_body(i, acc):
        jj = arrive(1, i)
        base = jj * size
        for t in range(8):
            at = slice(t * strip, (t + 1) * strip)
            v = beta * pd[jj, at, :] - pg[jj, at, :]
            acc = acc + fold(v * v)
            if t == 0:
                first_q, second_q, third_q, fourth_q = unpack_diagonal(v)
                store(base, base, first_q)
                store(base, base + strip, second_q)
                store(base + strip, base, third_q)
                store(base + strip, base + strip, fourth_q)
            elif t == 7:
                low_half = jj < blocks // 2
                v = jnp.where(low_half, v, -v)
                high_block = jnp.where(low_half, jj + blocks // 2, jj) * size + jnp.where(low_half, 0, strip)
                low_block = jnp.where(low_half, jj, jj - blocks // 2) * size
                store(high_block, low_block, v)
                store(low_block, high_block, -v.T)
            else:
                row = lax.rem(jj + (t + 1) // 2, blocks) * size + (t + 1) % 2 * strip
                store(row, base, v)
                store(base, row, -v.T)
        return acc

    dir_square = 2.0 * jnp.sum(lax.fori_loop(0, blocks, dir_body, zero))
    scale = STEP_SCALE / jnp.sqrt(jnp.full((1, size), 1.0 + dir_square / order, jnp.float32))

    tile = min(1024, order)
    own_cols = pl.ds(pl.multiple_of(own_block * size, size), size)

    def eye_rows(start, count):
        rid = lax.broadcasted_iota(jnp.int32, (count, size), 0) + start
        cid = lax.broadcasted_iota(jnp.int32, (count, size), 1) + own_block * size
        return (rid == cid).astype(jnp.float32)

    def first(i, carry):
        start = pl.multiple_of(i * size, size)
        rows = pl.ds(start, size)
        a = ahi[rows, own_cols].astype(jnp.float32) + alo[rows, own_cols].astype(jnp.float32)
        high, low = split_bf16(eye_rows(start, size) + a * (scale / TAYLOR))
        hhi[0, rows, :] = high
        hlo[0, rows, :] = low
        return carry

    lax.fori_loop(0, order // size, first, 0)

    def step(counter, carry):
        now = lax.rem(counter, 2)
        divisor = (TAYLOR - 1 - counter).astype(jnp.float32)
        inverse = scale / jnp.full((1, size), divisor, jnp.float32)
        bh = hhi[now]
        bl = hlo[now]

        def rows_body(i, c):
            start = pl.multiple_of(i * tile, tile)
            rows = pl.ds(start, tile)
            ah, al = ahi[rows, :], alo[rows, :]
            value = eye_rows(start, tile) + (dot(ah, bh) + dot(ah, bl) + dot(al, bh)) * inverse

            @pl.when(counter < TAYLOR - 2)
            def _():
                high, low = split_bf16(value)
                hhi[1 - now, rows, :] = high
                hlo[1 - now, rows, :] = low

            @pl.when(counter == TAYLOR - 2)
            def _():
                exp_out[rows, :] = value

            return c

        return lax.fori_loop(0, order // tile, rows_body, carry)

    lax.fori_loop(0, TAYLOR - 1, step, 0)


def output_kernel(ids, beta, dprev, *refs):
    g_in = refs[:-4]
    grad_out, dir_out, pg, sem = refs[-4:]
    r, z = ids[1], ids[2]
    blocks, _, size = pg.shape
    per_core = grad_out.shape[0] // size
    per_chip = grad_out.shape[1] // size
    for c in group_copies(ids, g_in, pg, sem, terms_place(ids)):
        c.start()
    for c in group_copies(ids, g_in, pg, sem, terms_place(ids)):
        c.wait()

    def out_body(t, carry):
        i, jx = lax.div(t, per_chip), lax.rem(t, per_chip)
        rb, cb = r * per_core + i, z * per_chip + jx
        o = lax.rem(rb - cb + blocks, blocks)
        rows = pl.ds(pl.multiple_of(i * size, size), size)
        cols = pl.ds(pl.multiple_of(jx * size, size), size)

        n = size // 2

        @pl.when(o == 0)
        def _():
            first_q, second_q, third_q, fourth_q = unpack_diagonal(pg[cb, :n, :])
            grad_out[rows, cols] = jnp.concatenate(
                [jnp.concatenate([first_q, second_q], axis=1), jnp.concatenate([third_q, fourth_q], axis=1)], axis=0)

        @pl.when((o > 0) & (o < 4))
        def _():
            grad_out[rows, cols] = pg[cb, pl.ds(pl.multiple_of(o * size - n, n), size), :]

        @pl.when(o > 4)
        def _():
            grad_out[rows, cols] = -pg[rb, pl.ds(pl.multiple_of((blocks - o) * size - n, n), size), :].T

        @pl.when((o == 4) & (rb > cb))
        def _():
            grad_out[rows, cols] = jnp.concatenate([pg[cb, 7 * n:, :], -pg[rb, 7 * n:, :]], axis=0)

        @pl.when((o == 4) & (rb < cb))
        def _():
            grad_out[rows, cols] = jnp.concatenate([-pg[rb, 7 * n:, :], pg[cb, 7 * n:, :]], axis=0).T

        dir_out[rows, cols] = beta[0, 0] * dprev[rows, cols] - grad_out[rows, cols]
        return carry

    lax.fori_loop(0, per_core * per_chip, out_body, 0)


def trial_kernel(ids, exp_lo, exp_hi, m0, m1, m2, m3, out, ehi, elo, mbuf, sem):
    r, z = ids[1], ids[2]
    half = exp_lo.shape[0]
    width = exp_lo.shape[1]
    size = m0.shape[2]
    blocks = 2 * half // size
    work = [(i, p) for i in range(4) for p in range(2)]
    sources = (m0, m1, m2, m3)

    def copy(n):
        i, p = work[n]
        return pltpu.make_async_copy(sources[i].at[p], mbuf.at[n % 3], sem.at[n % 3])

    copy(0).start()
    copy(1).start()
    for h, ref in enumerate((exp_lo, exp_hi)):
        high, low = split_bf16(ref[...])
        ehi[h * half:(h + 1) * half, :] = high
        elo[h * half:(h + 1) * half, :] = low
    totals = [jnp.zeros((8, width), jnp.float32) for _ in range(2)]
    for n, (i, p) in enumerate(work):
        if n + 2 < len(work):
            copy(n + 2).start()
        copy(n).wait()
        chip = z if i < 2 else jnp.bitwise_xor(z, 1)
        j = chip * 2 + (r if i % 2 == 0 else 1 - r)
        own = pl.ds(pl.multiple_of(j * size, size), size)
        bh, bl = ehi[own, :], elo[own, :]
        for o in range(5):
            high, low = split_bf16(mbuf[n % 3, o])
            z_o = dot(high, bh) + dot(high, bl) + dot(low, bh)
            at = pl.ds(pl.multiple_of(lax.rem(j + o, blocks) * size, size), size)
            e = ehi[at, :].astype(jnp.float32) + elo[at, :].astype(jnp.float32)
            term = jnp.sum((e * z_o).reshape(-1, 8, width), axis=0)
            totals[p] = totals[p] + (term if o in (0, 4) else 2.0 * term)
    out[...] = jnp.concatenate([jnp.sum(t, axis=0, keepdims=True) for t in totals], axis=0)


def lookup_weights(bvec_index, weight_table):
    table_slots = jnp.arange(weight_table.shape[0], dtype=jnp.int32)
    return jnp.sum(
        jnp.where(table_slots[None, :] == bvec_index[:, None], weight_table[None, :], 0.0), axis=1
    )


def paired(counts, m_matrices, bvec_index, weight_table, grad_prev, dir_prev):
    n_b, n_row, n_col = counts
    local_rows, local_cols = m_matrices.shape[2], m_matrices.shape[3]
    order = local_rows * n_row
    size = local_cols // n_row
    b, r, z = (lax.axis_index(a).astype(jnp.int32) for a in AXES)
    parity = jnp.bitwise_xor(b, b >> 1) & 1
    own_block = (z % 2) * 4 + parity * 2 + r
    ids = jnp.stack([b, r, z, own_block, parity]).astype(jnp.int32)

    def send(x, where):
        pairs = []
        for bb in range(n_b):
            for rr in range(n_row):
                for zz in range(n_col):
                    tb, tr, tz = where(bb, rr, zz)
                    pairs.append(((bb * n_row + rr) * n_col + zz, (tb * n_row + tr) * n_col + tz))
        return lax.ppermute(x, AXES, pairs)

    core = lambda bb, rr, zz: (bb, 1 - rr, zz)
    over_b = lambda k: (lambda bb, rr, zz: (bb ^ k, rr, zz))
    over_z = lambda s: (lambda bb, rr, zz: (bb, rr, (zz + s) % n_col))
    flip_z = lambda k: (lambda bb, rr, zz: (bb, rr, zz ^ k))

    weight_all = lookup_weights(bvec_index, weight_table)
    weight_own = lax.dynamic_slice_in_dim(weight_all, b, 1)
    m = m_matrices[0]

    d_oth = send(dir_prev, core)
    start = (z % 2) * local_cols
    square = lax.dynamic_slice_in_dim(m, start, local_cols, 1)
    holder = (z // 2 == r)
    eye = jnp.eye(local_cols, dtype=jnp.bool_)
    own_diag = jnp.sum(jnp.where(eye & holder, square, 0.0), axis=1)
    prev_part = jnp.sum(grad_prev * grad_prev)
    packet = jnp.concatenate([own_diag, jnp.full((1, local_cols), prev_part)], axis=0)
    packet = packet + send(packet, core)
    m_oth = send(m, core)
    diags = jnp.stack([packet] + [send(packet, over_z(s)) for s in range(1, n_col)])
    prev_square = jnp.sum(diags[:, 2, :1], axis=0)
    spread_own = weight_own[0] * jnp.sum(1.0 - diags[:, 0] ** 2 - diags[:, 1] ** 2) / order

    quarter = jax.ShapeDtypeStruct((size, size), jnp.float32)
    d_own, d_half = pl.pallas_call(
        quarter_kernel, out_shape=[jax.ShapeDtypeStruct((n, size, size), jnp.float32) for n in (4, 2)],
        in_specs=[SMEM, ANY, ANY], out_specs=[VMEM] * 2,
        scratch_shapes=[pltpu.VMEM((5, size, size), jnp.float32), pltpu.SemaphoreType.DMA((5,))],
        cost_estimate=pl.CostEstimate(flops=0, bytes_accessed=1 << 20, transcendentals=0),
    )(ids, dir_prev, d_oth)
    d_by_z = {s: send(d_half, over_z(s)) for s in (1, 3, 2)}
    terms = pl.pallas_call(
        term_kernel, out_shape=[quarter] * 4 + [jax.ShapeDtypeStruct((2, 5, size, size), jnp.float32)],
        in_specs=[SMEM, SMEM, VMEM, ANY, ANY], out_specs=[ANY] * 5,
        scratch_shapes=[pltpu.VMEM((5, size, size), jnp.float32), pltpu.VMEM((5, size, size), jnp.float32),
                        pltpu.VMEM((4, size, size), jnp.float32),
                        pltpu.SemaphoreType.DMA((2, 5)), pltpu.SemaphoreType.DMA((4,)),
                        pltpu.SemaphoreType.DMA((2, 5))],
        cost_estimate=pl.CostEstimate(flops=10**9, bytes_accessed=1 << 22, transcendentals=0),
    )(ids, weight_own, diags, m, m_oth)
    parts = [send(terms[k], over_b(k)) for k in range(1, n_b)]
    g_quarter = ((terms[0] + parts[0]) + parts[1]) + parts[2]

    d_groups = [d_own] + [
        jnp.concatenate([d_by_z[s], send(d_by_z[s][:1], over_b(1)), send(d_by_z[s][1:], over_b(2))])
        for s in range(1, n_col)
    ]
    d_groups = d_groups + [send(g, core) for g in d_groups]
    g_by_z = {0: g_quarter}
    for s in (1, 3, 2):
        g_by_z[s] = send(g_quarter, over_z(s))
    g_groups = []
    for s in range(n_col):
        piece = g_by_z[s]
        over_x = send(piece, over_b(1))
        over_y = send(piece, over_b(2))
        if s in (1, 2):
            across = send(over_y, over_b(1))
        else:
            across = send(over_x, over_b(2))
        g_groups.append(jnp.stack([piece, over_x, over_y, across]))
    g_groups = g_groups + [send(g, core) for g in g_groups]
    chosen_z = send(terms[4], flip_z(1))

    f32 = jnp.float32
    held = pltpu.VMEM((2 * n_col, 4 * size, size), f32)
    beta, exp_own = pl.pallas_call(
        solve_kernel,
        out_shape=[jax.ShapeDtypeStruct((8, 128), f32), jax.ShapeDtypeStruct((order, size), f32)],
        in_specs=[SMEM, SMEM] + [ANY] * (4 * n_col), out_specs=[VMEM] * 2,
        scratch_shapes=[held, held,
                        pltpu.VMEM((order, order), jnp.bfloat16), pltpu.VMEM((order, order), jnp.bfloat16),
                        pltpu.VMEM((2, order, size), jnp.bfloat16), pltpu.VMEM((2, order, size), jnp.bfloat16),
                        pltpu.SemaphoreType.DMA((2, 2 * n_col))],
        compiler_params=pltpu.CompilerParams(vmem_limit_bytes=VMEM_LIMIT),
        cost_estimate=pl.CostEstimate(flops=7 * 3 * 2 * order * order * size, bytes_accessed=1 << 25, transcendentals=0),
    )(ids, prev_square, *g_groups, *d_groups)
    outputs = pl.pallas_call(
        output_kernel, out_shape=[jax.ShapeDtypeStruct((local_rows, local_cols), f32)] * 2,
        in_specs=[SMEM, SMEM, VMEM] + [ANY] * (2 * n_col), out_specs=[VMEM] * 2,
        scratch_shapes=[held, pltpu.SemaphoreType.DMA((2 * n_col,))],
        compiler_params=pltpu.CompilerParams(vmem_limit_bytes=VMEM_LIMIT),
        cost_estimate=pl.CostEstimate(flops=10**9, bytes_accessed=1 << 24, transcendentals=0),
    )
    grad, direction = outputs(ids, beta[:1], dir_prev, *g_groups)

    exp_own, chosen_z = lax.optimization_barrier((exp_own, chosen_z))
    chosen_set = (terms[4], send(terms[4], core), chosen_z, send(chosen_z, core))
    top, bottom = exp_own[:order // 2], exp_own[order // 2:]
    top_in = send(top, over_b(1))
    bottom_in = send(bottom, over_b(2))

    def trial(lo, hi):
        return pl.pallas_call(
            trial_kernel, out_shape=jax.ShapeDtypeStruct((2, size), f32),
            in_specs=[SMEM, VMEM, VMEM] + [ANY] * 4, out_specs=VMEM,
            scratch_shapes=[pltpu.VMEM((order, size), jnp.bfloat16), pltpu.VMEM((order, size), jnp.bfloat16),
                            pltpu.VMEM((3, 5, size, size), f32), pltpu.SemaphoreType.DMA((3,))],
            compiler_params=pltpu.CompilerParams(vmem_limit_bytes=VMEM_LIMIT // 2),
            cost_estimate=pl.CostEstimate(flops=3 * 2 * order * order * size, bytes_accessed=1 << 24, transcendentals=0),
        )(ids, lo, hi, *chosen_set)

    t_own = trial(top, bottom)
    top_in, bottom_in, grad, direction = lax.optimization_barrier((top_in, bottom_in, grad, direction))
    t_in = trial(top_in, bottom_in)

    def ordered(bit, mine, theirs):
        return jnp.where(bit == 0, jnp.stack([mine, theirs]), jnp.stack([theirs, mine]))

    t = ordered(parity, t_own, t_in)
    t = t + send(t, flip_z(2))
    t = ordered(z % 2, t, send(t, flip_z(1)))
    t = ordered(r, t, send(t, core))
    t = jnp.transpose(t, (3, 1, 2, 0, 4)).reshape(2, order)
    t = jnp.concatenate([t, jnp.full((1, order), spread_own)], axis=0)
    t = ordered(b & 1, t, send(t, over_b(1)))
    t = ordered(b >> 1, t, send(t, over_b(2))).reshape(n_b, 3, order)
    trial_diag = t[:, :2]
    spread = jnp.sum(t[:, 2, 0])
    trial_spread = (
        jnp.sum(weight_all[:, None] * (1.0 - trial_diag[:, 0] ** 2 - trial_diag[:, 1] ** 2)) / order
    )
    return (spread, trial_spread, grad, direction, trial_diag)


def product(left, right):
    return jnp.dot(left, right, precision=HIGHEST, preferred_element_type=jnp.float32)


def shards(m_matrices, bvec_index, weight_table, grad_prev, dir_prev):
    per_group = m_matrices.shape[0]
    local_rows = m_matrices.shape[2]
    local_cols = m_matrices.shape[3]
    matrix_order = local_rows * lax.axis_size("row")
    group_index = lax.axis_index("bvec")
    row_start = lax.axis_index("row") * local_rows
    col_start = lax.axis_index("col") * local_cols
    weight_all = lookup_weights(bvec_index, weight_table)
    weight_own = lax.dynamic_slice_in_dim(weight_all, group_index * per_group, per_group)
    row_ids = row_start + jnp.arange(local_rows, dtype=jnp.int32)
    col_ids = col_start + jnp.arange(local_cols, dtype=jnp.int32)
    on_diag = (row_ids[:, None] == col_ids[None, :]).astype(jnp.float32)
    own_diag = jnp.sum(m_matrices * on_diag, axis=2)
    share_diag = lax.psum(own_diag, "row")
    diagonal = lax.all_gather(share_diag, "col", axis=2, tiled=True)
    row_diag = lax.dynamic_slice_in_dim(diagonal, row_start, local_rows, 2)
    spread_own = (
        jnp.sum(weight_own[:, None] * (1.0 - diagonal[:, 0] ** 2 - diagonal[:, 1] ** 2))
        / matrix_order
    )
    leader = (lax.axis_index("row") == 0) & (lax.axis_index("col") == 0)
    spread_term = jnp.where(leader, spread_own, 0.0)
    differ = row_diag[:, :, :, None] - share_diag[:, :, None, :]
    weighted = 2.0 * weight_own[:, None, None] * jnp.sum(m_matrices * differ, axis=1)
    grad_part = jnp.sum(weighted, axis=0)
    gradient = lax.psum(grad_part, "bvec")
    counted = jnp.where(group_index == 0, 1.0, 0.0)
    grad_square = counted * jnp.sum(gradient * gradient)
    prev_square = counted * jnp.sum(grad_prev * grad_prev)
    cross_term = counted * jnp.sum(gradient * dir_prev)
    dir_square = counted * jnp.sum(dir_prev * dir_prev)
    totals = lax.psum(
        (spread_term, grad_square, prev_square, cross_term, dir_square), ("bvec", "row", "col")
    )
    spread = totals[0]
    beta_factor = totals[1] / (1.0 + totals[2])
    direction = beta_factor * dir_prev - gradient
    dir_norm = jnp.maximum(
        totals[1] - 2.0 * beta_factor * totals[3] + beta_factor * beta_factor * totals[4], 0.0
    )
    generator = STEP_SCALE * direction / jnp.sqrt(1.0 + dir_norm / matrix_order)
    block_ids = col_start + jnp.arange(local_cols, dtype=jnp.int32)
    eye_block = (row_ids[:, None] == block_ids[None, :]).astype(jnp.float32)
    horner_start = eye_block + generator / TAYLOR
    columns = lax.all_gather(generator, "row", axis=0, tiled=True)

    def accumulate(section):
        return product(section, columns)

    def horner_step(counter, current):
        folded = accumulate(lax.all_gather(current, "col", axis=1, tiled=True))
        divisor = (TAYLOR - 1 - counter).astype(jnp.float32)
        return eye_block + folded / divisor

    expmap = lax.fori_loop(0, TAYLOR - 1, horner_step, horner_start)
    expmap_cols = lax.all_gather(expmap, "row", axis=0, tiled=True)
    section = lax.all_gather(m_matrices, "col", axis=3, tiled=True)
    flattened = section.reshape((-1, section.shape[3]))
    rotated = product(flattened, expmap_cols).reshape(
        jnp.zeros(m_matrices.shape, jnp.float32).shape
    )
    trial_part = jnp.sum(expmap[None, None] * rotated, axis=2)
    trial_share = lax.psum(trial_part, "row")
    trial_group = lax.all_gather(trial_share, "col", axis=2, tiled=True)
    trial_diag = lax.all_gather(trial_group, "bvec", axis=0, tiled=True)
    trial_spread = (
        jnp.sum(weight_all[:, None] * (1.0 - trial_diag[:, 0] ** 2 - trial_diag[:, 1] ** 2))
        / matrix_order
    )
    return (spread, trial_spread, gradient, direction, trial_diag)


def solution(mesh):
    placed = (P("bvec", None, "row", "col"), P(), P(), P("row", "col"), P("row", "col"))
    counts = tuple(mesh.shape[a] for a in AXES)
    special = counts == (4, 2, 4)

    def named(*args):
        return paired(counts, *args)

    return jax.shard_map(
        named if special else shards,
        mesh=mesh,
        in_specs=placed,
        out_specs=(P(), P(), P("row", "col"), P("row", "col"), P()),
        check_vma=False,
    )
```

```python
import jax
import jax.numpy as jnp
from jax import lax
from jax.experimental import pallas as pl
from jax.experimental.pallas import tpu as pltpu
from jax.sharding import PartitionSpec as P


TAYLOR = 8
STEP_SCALE = 1.75
HIGHEST = lax.Precision.HIGHEST
AXES = ("bvec", "row", "col")
ANY = pl.BlockSpec(memory_space=pl.ANY)
SMEM = pl.BlockSpec(memory_space=pltpu.SMEM)
VMEM = pl.BlockSpec(memory_space=pltpu.VMEM)
VMEM_LIMIT = 62 * 1024 * 1024


def split_bf16(x):
    high = x.astype(jnp.bfloat16)
    low = (x - high.astype(jnp.float32)).astype(jnp.bfloat16)
    return high, low


def dot(a, b):
    return jnp.dot(a, b, preferred_element_type=jnp.float32)


def above(n):
    return lax.broadcasted_iota(jnp.int32, (n, n), 1) > lax.broadcasted_iota(jnp.int32, (n, n), 0)


def pack_block(part, o, value, low_half):
    n = value.shape[0] // 2

    def put(i, rows):
        part[i // 2, i % 2 * n:(i % 2 + 1) * n, :] = rows

    if o == 0:
        mixed = jnp.where(above(n), value[:n, :n], value[n:, n:])
        put(0, jnp.concatenate([mixed, value[:n, n:]], axis=1))
    elif o == 4:
        put(7, jnp.where(low_half, value[:n, :], value[:, n:].T))
    else:
        put(2 * o - 1, value[:n])
        put(2 * o, value[n:])


def unpack_diagonal(rows):
    n = rows.shape[0]
    mixed, corner = rows[:, :n], rows[:, n:]
    upper = jnp.where(above(n), mixed, 0.0)
    below = lax.broadcasted_iota(jnp.int32, (n, n), 1) < lax.broadcasted_iota(jnp.int32, (n, n), 0)
    lower = jnp.where(below, mixed, 0.0)
    return upper - upper.T, corner, -corner.T, lower - lower.T


def packet_kernel(ids, m, prev, out, square, gprev, sem):
    r, z = ids[1], ids[2]
    n = square.shape[1]
    per_core = m.shape[1] // n
    rows = pl.ds(pl.multiple_of(lax.rem(z, per_core) * n, n), n)
    squares = [pltpu.make_async_copy(m.at[p, rows, :], square.at[p], sem.at[p]) for p in range(2)]
    other = pltpu.make_async_copy(prev, gprev, sem.at[2])
    holder = lax.div(z, per_core) == r
    other.start()

    @pl.when(holder)
    def _():
        for c in squares:
            c.start()
        on_diag = lax.broadcasted_iota(jnp.int32, (n, n), 0) == lax.broadcasted_iota(jnp.int32, (n, n), 1)
        for p, c in enumerate(squares):
            c.wait()
            out[p:p + 1, :] = jnp.sum(jnp.where(on_diag, square[p], 0.0), axis=0, keepdims=True)

    @pl.when(jnp.logical_not(holder))
    def _():
        out[0:2, :] = jnp.zeros((2, n), jnp.float32)

    other.wait()
    g = gprev[...]
    total = jnp.sum(jnp.sum((g * g).reshape(-1, 8, n), axis=0))
    out[2:3, :] = jnp.full((1, n), total, jnp.float32)


def term_kernel(ids, weight, diags, own, other, o0, o1, o2, o3, chosen, mre, mim, part, sem, out_sem, chosen_sem):
    b, r, z = ids[0], ids[1], ids[2]
    size = mre.shape[-1]
    per_core = own.shape[1] // size
    blocks = 2 * per_core
    kept = mre.shape[0]
    per_chip = own.shape[2] // size
    groups = blocks // per_chip
    j = z * per_chip + r
    lanes = pl.ds(pl.multiple_of(r * size, size), size)
    for o in range(kept):
        block = lax.rem(j + o, blocks)
        rows = pl.ds(pl.multiple_of(lax.rem(block, per_core) * size, size), size)
        mine = lax.div(block, per_core) == r
        for ref, cond in ((own, mine), (other, jnp.logical_not(mine))):
            @pl.when(cond)
            def _(ref=ref, o=o, rows=rows):
                pltpu.make_async_copy(ref.at[0, rows, lanes], mre.at[o], sem.at[0, o]).start()
                pltpu.make_async_copy(ref.at[1, rows, lanes], mim.at[o], sem.at[1, o]).start()

    def piece(block, p):
        slot = lax.rem(z - lax.div(block, per_chip) + groups, groups)
        half = lax.rem(block, per_chip)
        row = diags[slot, pl.ds(p, 1), :]
        return jnp.where(half == 0, row[:, :size], row[:, size:])

    factor = 2.0 * weight[b]
    re_own, im_own = piece(j, 0), piece(j, 1)
    low_half = j < blocks // 2
    copies = []
    for o in range(kept):
        block = lax.rem(j + o, blocks)
        re_rows = jnp.broadcast_to(piece(block, 0), (size, size)).T
        im_rows = jnp.broadcast_to(piece(block, 1), (size, size)).T
        pltpu.make_async_copy(own.at[0, pl.ds(0, size), pl.ds(0, size)], mre.at[o], sem.at[0, o]).wait()
        pltpu.make_async_copy(own.at[0, pl.ds(0, size), pl.ds(0, size)], mim.at[o], sem.at[1, o]).wait()
        kept_copies = [pltpu.make_async_copy(buf.at[o], chosen.at[p, o], chosen_sem.at[p, o]) for p, buf in enumerate((mre, mim))]
        for copy in kept_copies:
            copy.start()
        copies += kept_copies
        value = factor * (mre[o] * (re_rows - re_own) + mim[o] * (im_rows - im_own))
        pack_block(part, o, value, low_half)
    for k, out in enumerate((o0, o1, o2, o3)):
        copy = pltpu.make_async_copy(part.at[jnp.bitwise_xor(b, k)], out, out_sem.at[k])
        copy.start()
        copies.append(copy)
    for copy in copies:
        copy.wait()


def quarter_kernel(ids, own, other, out, half, buf, sem):
    r, z, h = ids[1], ids[2], ids[4]
    size = buf.shape[2]
    per_core = own.shape[0] // size
    blocks = 2 * per_core
    per_chip = own.shape[1] // size
    j = z * per_chip + r
    lanes = pl.ds(pl.multiple_of(r * size, size), size)
    for o in range(5):
        block = lax.rem(j + o, blocks)
        rows = pl.ds(pl.multiple_of(lax.rem(block, per_core) * size, size), size)
        mine = lax.div(block, per_core) == r
        for ref, cond in ((own, mine), (other, jnp.logical_not(mine))):
            @pl.when(cond)
            def _(ref=ref, rows=rows, o=o):
                pltpu.make_async_copy(ref.at[rows, lanes], buf.at[o], sem.at[o]).start()
    for o in range(5):
        pltpu.make_async_copy(own.at[pl.ds(0, size), pl.ds(0, size)], buf.at[o], sem.at[o]).wait()
        pack_block(out, o, buf[o], j < blocks // 2)
    half[...] = jnp.where(h == 0, out[0:2], out[2:4])


def group_copies(ids, ins, dst, sem, place):
    r, z = ids[1], ids[2]
    groups = len(ins) // 2
    quarter = ins[0].shape[1]
    out = []
    for i, ref in enumerate(ins):
        s, c = i % groups, i // groups
        j = lax.rem(z - s + groups, groups) * 2 + (r if c == 0 else 1 - r)
        for k in range(4):
            rows = pl.ds(pl.multiple_of(place(s, k) * quarter, quarter), quarter)
            out.append(pltpu.make_async_copy(ref.at[k], dst.at[j, rows], sem.at[i]))
    return out


def terms_place(ids):
    return lambda s, k: jnp.bitwise_xor(ids[0], k)


def shared_place(ids):
    h = ids[4]
    return lambda s, k: k if s == 0 else (2 * h + k if k < 2 else 2 * (1 - h) + k - 2)


def solve_kernel(ids, prev_square, *refs):
    groups = (len(refs) - 11) // 4
    g_in, d_in = refs[:2 * groups], refs[2 * groups:4 * groups]
    beta_out, exp_a, exp_b, exp_c, pg, pd, ahi, alo, hhi, hlo, sem = refs[4 * groups:]
    own_block = ids[3]
    order = ahi.shape[0]
    blocks, _, size = pg.shape

    g_copies = group_copies(ids, g_in, pg, sem.at[0], terms_place(ids))
    d_copies = group_copies(ids, d_in, pd, sem.at[1], shared_place(ids))
    for c in g_copies + d_copies:
        c.start()
    strip = size // 2

    def fold(x):
        return jnp.sum(x.reshape(-1, 8, size), axis=0)

    quarter = g_in[0].shape[1]

    def arrive(which, i):
        for k in range(4):
            at = pl.ds(k * quarter, quarter)
            pltpu.make_async_copy(g_in[0].at[k], pg.at[0, at], sem.at[which, i]).wait()
        core = lax.div(i, groups)
        column = lax.rem(ids[2] - lax.rem(i, groups) + groups, groups) * 2
        return column + jnp.where(core == 0, ids[1], 1 - ids[1])

    def norm_body(i, acc):
        jj = arrive(0, i)
        for t in range(0, pg.shape[1], size):
            v = pg[jj, t:t + size, :]
            acc = acc + fold(v * v)
        return acc

    zero = jnp.zeros((8, size), jnp.float32)
    beta = 2.0 * jnp.sum(lax.fori_loop(0, blocks, norm_body, zero)) / (1.0 + prev_square[0])
    beta_out[...] = jnp.full(beta_out.shape, beta, jnp.float32)

    def store(row, col, v):
        high, low = split_bf16(v)
        rows = pl.ds(pl.multiple_of(row, strip), v.shape[0])
        cols = pl.ds(pl.multiple_of(col, strip), v.shape[1])
        ahi[rows, cols] = high
        alo[rows, cols] = low

    def dir_body(i, acc):
        jj = arrive(1, i)
        base = jj * size
        for t in range(8):
            at = slice(t * strip, (t + 1) * strip)
            v = beta * pd[jj, at, :] - pg[jj, at, :]
            acc = acc + fold(v * v)
            if t == 0:
                first_q, second_q, third_q, fourth_q = unpack_diagonal(v)
                store(base, base, first_q)
                store(base, base + strip, second_q)
                store(base + strip, base, third_q)
                store(base + strip, base + strip, fourth_q)
            elif t == 7:
                low_half = jj < blocks // 2
                v = jnp.where(low_half, v, -v)
                high_block = jnp.where(low_half, jj + blocks // 2, jj) * size + jnp.where(low_half, 0, strip)
                low_block = jnp.where(low_half, jj, jj - blocks // 2) * size
                store(high_block, low_block, v)
                store(low_block, high_block, -v.T)
            else:
                row = lax.rem(jj + (t + 1) // 2, blocks) * size + (t + 1) % 2 * strip
                store(row, base, v)
                store(base, row, -v.T)
        return acc

    dir_square = 2.0 * jnp.sum(lax.fori_loop(0, blocks, dir_body, zero))
    scale = STEP_SCALE / jnp.sqrt(jnp.full((1, size), 1.0 + dir_square / order, jnp.float32))

    tile = min(1024, order)
    own_cols = pl.ds(pl.multiple_of(own_block * size, size), size)

    def eye_rows(start, count):
        rid = lax.broadcasted_iota(jnp.int32, (count, size), 0) + start
        cid = lax.broadcasted_iota(jnp.int32, (count, size), 1) + own_block * size
        return (rid == cid).astype(jnp.float32)

    def first(i, carry):
        start = pl.multiple_of(i * size, size)
        rows = pl.ds(start, size)
        a = ahi[rows, own_cols].astype(jnp.float32) + alo[rows, own_cols].astype(jnp.float32)
        high, low = split_bf16(eye_rows(start, size) + a * (scale / TAYLOR))
        hhi[0, rows, :] = high
        hlo[0, rows, :] = low
        return carry

    lax.fori_loop(0, order // size, first, 0)

    def step(counter, carry):
        now = lax.rem(counter, 2)
        divisor = (TAYLOR - 1 - counter).astype(jnp.float32)
        inverse = scale / jnp.full((1, size), divisor, jnp.float32)
        bh = hhi[now]
        bl = hlo[now]

        def rows_body(i, c):
            start = pl.multiple_of(i * tile, tile)
            rows = pl.ds(start, tile)
            ah, al = ahi[rows, :], alo[rows, :]
            value = eye_rows(start, tile) + (dot(ah, bh) + dot(ah, bl) + dot(al, bh)) * inverse

            @pl.when(counter < TAYLOR - 2)
            def _():
                high, low = split_bf16(value)
                hhi[1 - now, rows, :] = high
                hlo[1 - now, rows, :] = low

            for t in range(order // tile):
                @pl.when((counter == TAYLOR - 2) & (i == t))
                def _(t=t):
                    begin = 0
                    for ref in (exp_a, exp_b, exp_c):
                        end = begin + ref.shape[0]
                        lo, hi = max(begin, t * tile), min(end, (t + 1) * tile)
                        if lo < hi:
                            ref[lo - begin:hi - begin, :] = value[lo - t * tile:hi - t * tile]
                        begin = end
            return c

        return lax.fori_loop(0, order // tile, rows_body, carry)

    lax.fori_loop(0, TAYLOR - 1, step, 0)


def output_kernel(ids, beta, dprev, *refs):
    g_in = refs[:-4]
    grad_out, dir_out, pg, sem = refs[-4:]
    r, z = ids[1], ids[2]
    blocks, _, size = pg.shape
    per_core = grad_out.shape[0] // size
    per_chip = grad_out.shape[1] // size
    for c in group_copies(ids, g_in, pg, sem, terms_place(ids)):
        c.start()
    for c in group_copies(ids, g_in, pg, sem, terms_place(ids)):
        c.wait()

    def out_body(t, carry):
        i, jx = lax.div(t, per_chip), lax.rem(t, per_chip)
        rb, cb = r * per_core + i, z * per_chip + jx
        o = lax.rem(rb - cb + blocks, blocks)
        rows = pl.ds(pl.multiple_of(i * size, size), size)
        cols = pl.ds(pl.multiple_of(jx * size, size), size)

        n = size // 2

        @pl.when(o == 0)
        def _():
            first_q, second_q, third_q, fourth_q = unpack_diagonal(pg[cb, :n, :])
            grad_out[rows, cols] = jnp.concatenate(
                [jnp.concatenate([first_q, second_q], axis=1), jnp.concatenate([third_q, fourth_q], axis=1)], axis=0)

        @pl.when((o > 0) & (o < 4))
        def _():
            grad_out[rows, cols] = pg[cb, pl.ds(pl.multiple_of(o * size - n, n), size), :]

        @pl.when(o > 4)
        def _():
            grad_out[rows, cols] = -pg[rb, pl.ds(pl.multiple_of((blocks - o) * size - n, n), size), :].T

        @pl.when((o == 4) & (rb > cb))
        def _():
            grad_out[rows, cols] = jnp.concatenate([pg[cb, 7 * n:, :], -pg[rb, 7 * n:, :]], axis=0)

        @pl.when((o == 4) & (rb < cb))
        def _():
            grad_out[rows, cols] = jnp.concatenate([-pg[rb, 7 * n:, :], pg[cb, 7 * n:, :]], axis=0).T

        dir_out[rows, cols] = beta[0:1, 0:1] * dprev[rows, cols] - grad_out[rows, cols]
        return carry

    lax.fori_loop(0, per_core * per_chip, out_body, 0)


def trial_kernel(ids, exp_a, exp_b, exp_c, m0, m1, m2, m3, out, e, ehi, elo, mbuf, sem):
    r, z = ids[1], ids[2]
    width = exp_a.shape[1]
    size = m0.shape[2]
    blocks = e.shape[0] // size
    work = [(i, p) for i in range(4) for p in range(2)]
    sources = (m0, m1, m2, m3)

    def copy(n):
        i, p = work[n]
        return pltpu.make_async_copy(sources[i].at[p], mbuf.at[n % 3], sem.at[n % 3])

    copy(0).start()
    copy(1).start()
    begin = 0
    for ref in (exp_a, exp_b, exp_c):
        high, low = split_bf16(ref[...])
        rows = slice(begin, begin + ref.shape[0])
        e[rows, :] = ref[...]
        ehi[rows, :] = high
        elo[rows, :] = low
        begin += ref.shape[0]
    totals = [jnp.zeros((8, width), jnp.float32) for _ in range(2)]
    for n, (i, p) in enumerate(work):
        if n + 2 < len(work):
            copy(n + 2).start()
        copy(n).wait()
        chip = z if i < 2 else jnp.bitwise_xor(z, 1)
        j = chip * 2 + (r if i % 2 == 0 else 1 - r)
        own = pl.ds(pl.multiple_of(j * size, size), size)
        bh, bl = ehi[own, :], elo[own, :]
        for o in range(5):
            high, low = split_bf16(mbuf[n % 3, o])
            value = dot(high, bh) + dot(high, bl) + dot(low, bh)
            at = pl.ds(pl.multiple_of(lax.rem(j + o, blocks) * size, size), size)
            term = jnp.sum((e[at, :] * value).reshape(-1, 8, width), axis=0)
            totals[p] = totals[p] + (term if o in (0, 4) else 2.0 * term)
    out[...] = jnp.concatenate([jnp.sum(t, axis=0, keepdims=True) for t in totals], axis=0)


def closing_kernel(ids, weights, *refs):
    diag_out, sums = refs[-2:]
    order = diag_out.shape[2]
    spread, trial = jnp.float32(0.0), jnp.float32(0.0)
    for k, ref in enumerate(refs[:-2]):
        group = jnp.bitwise_xor(ids[0], k)
        re, im = ref[0:1, :], ref[1:2, :]
        diag_out[group] = ref[0:2, :]
        spread = spread + ref[2, 0]
        trial = trial + weights[group] * jnp.sum(1.0 - re * re - im * im)
    sums[0] = spread
    sums[1] = trial / order


def lookup_weights(bvec_index, weight_table):
    table_slots = jnp.arange(weight_table.shape[0], dtype=jnp.int32)
    return jnp.sum(
        jnp.where(table_slots[None, :] == bvec_index[:, None], weight_table[None, :], 0.0), axis=1
    )


def paired(counts, m_matrices, bvec_index, weight_table, grad_prev, dir_prev):
    n_b, n_row, n_col = counts
    local_rows, local_cols = m_matrices.shape[2], m_matrices.shape[3]
    order = local_rows * n_row
    size = local_cols // n_row
    b, r, z = (lax.axis_index(a).astype(jnp.int32) for a in AXES)
    parity = jnp.bitwise_xor(b, b >> 1) & 1
    half_id = jnp.bitwise_xor(parity, z >> 1) & 1
    own_block = (z % 2) * 4 + half_id * 2 + r
    ids = jnp.stack([b, r, z, own_block, parity]).astype(jnp.int32)

    def send(x, where):
        pairs = []
        for bb in range(n_b):
            for rr in range(n_row):
                for zz in range(n_col):
                    tb, tr, tz = where(bb, rr, zz)
                    pairs.append(((bb * n_row + rr) * n_col + zz, (tb * n_row + tr) * n_col + tz))
        return lax.ppermute(x, AXES, pairs)

    core = lambda bb, rr, zz: (bb, 1 - rr, zz)
    over_b = lambda k: (lambda bb, rr, zz: (bb ^ k, rr, zz))
    over_z = lambda s: (lambda bb, rr, zz: (bb, rr, (zz + s) % n_col))
    flip_z = lambda k: (lambda bb, rr, zz: (bb, rr, zz ^ k))

    weight_all = lookup_weights(bvec_index, weight_table)
    weight_own = lax.dynamic_slice_in_dim(weight_all, b, 1)
    m = m_matrices[0]

    d_oth = send(dir_prev, core)
    packet = pl.pallas_call(
        packet_kernel, out_shape=jax.ShapeDtypeStruct((3, local_cols), jnp.float32),
        in_specs=[SMEM, ANY, ANY], out_specs=VMEM,
        scratch_shapes=[pltpu.VMEM((2, local_cols, local_cols), jnp.float32), pltpu.VMEM(grad_prev.shape, jnp.float32),
                        pltpu.SemaphoreType.DMA((3,))],
        cost_estimate=pl.CostEstimate(flops=10**6, bytes_accessed=1 << 22, transcendentals=0),
    )(ids, m, grad_prev)
    packet = packet + send(packet, core)
    m_oth = send(m, core)
    d_own, d_half = pl.pallas_call(
        quarter_kernel, out_shape=[jax.ShapeDtypeStruct((n, size, size), jnp.float32) for n in (4, 2)],
        in_specs=[SMEM, ANY, ANY], out_specs=[VMEM] * 2,
        scratch_shapes=[pltpu.VMEM((5, size, size), jnp.float32), pltpu.SemaphoreType.DMA((5,))],
        cost_estimate=pl.CostEstimate(flops=0, bytes_accessed=1 << 20, transcendentals=0),
    )(ids, dir_prev, d_oth)
    packet, d_half = lax.optimization_barrier((packet, d_half))
    diags = jnp.stack([packet] + [send(packet, over_z(s)) for s in range(1, n_col)])
    prev_square = jnp.sum(diags[:, 2, :1], axis=0)
    spread_own = weight_own[0] * jnp.sum(1.0 - diags[:, 0] ** 2 - diags[:, 1] ** 2) / order

    quarter = jax.ShapeDtypeStruct((size, size), jnp.float32)
    d_by_z = {s: send(d_half, over_z(s)) for s in (1, 3, 2)}
    terms = pl.pallas_call(
        term_kernel, out_shape=[quarter] * 4 + [jax.ShapeDtypeStruct((2, 5, size, size), jnp.float32)],
        in_specs=[SMEM, SMEM, VMEM, ANY, ANY], out_specs=[ANY] * 5,
        scratch_shapes=[pltpu.VMEM((5, size, size), jnp.float32), pltpu.VMEM((5, size, size), jnp.float32),
                        pltpu.VMEM((4, size, size), jnp.float32),
                        pltpu.SemaphoreType.DMA((2, 5)), pltpu.SemaphoreType.DMA((4,)),
                        pltpu.SemaphoreType.DMA((2, 5))],
        cost_estimate=pl.CostEstimate(flops=10**9, bytes_accessed=1 << 22, transcendentals=0),
    )(ids, weight_all, diags, m, m_oth)
    parts = [send(terms[k], over_b(k)) for k in range(1, n_b)]
    g_quarter = ((terms[0] + parts[0]) + parts[1]) + parts[2]

    d_groups = [d_own] + [
        jnp.concatenate([d_by_z[s], send(d_by_z[s][:1], over_b(1)), send(d_by_z[s][1:], over_b(2))])
        for s in range(1, n_col)
    ]
    d_groups = d_groups + [send(g, core) for g in d_groups]
    g_by_z = {0: g_quarter}
    for s in (1, 3, 2):
        g_by_z[s] = send(g_quarter, over_z(s))
    g_groups = []
    for s in range(n_col):
        piece = g_by_z[s]
        over_x = send(piece, over_b(1))
        over_y = send(piece, over_b(2))
        if s in (1, 2):
            across = send(over_y, over_b(1))
        else:
            across = send(over_x, over_b(2))
        g_groups.append(jnp.stack([piece, over_x, over_y, across]))
    g_groups = g_groups + [send(g, core) for g in g_groups]
    chosen_z = send(terms[4], flip_z(1))

    f32 = jnp.float32
    held = pltpu.VMEM((2 * n_col, 4 * size, size), f32)
    by_plane = 13 * order // 32 // 8 * 8
    shares = (by_plane, by_plane, order - 2 * by_plane)
    beta, *exp_own = pl.pallas_call(
        solve_kernel,
        out_shape=[jax.ShapeDtypeStruct((8, 128), f32)] + [jax.ShapeDtypeStruct((n, size), f32) for n in shares],
        in_specs=[SMEM, SMEM] + [ANY] * (4 * n_col), out_specs=[VMEM] * 4,
        scratch_shapes=[held, held,
                        pltpu.VMEM((order, order), jnp.bfloat16), pltpu.VMEM((order, order), jnp.bfloat16),
                        pltpu.VMEM((2, order, size), jnp.bfloat16), pltpu.VMEM((2, order, size), jnp.bfloat16),
                        pltpu.SemaphoreType.DMA((2, 2 * n_col))],
        compiler_params=pltpu.CompilerParams(vmem_limit_bytes=VMEM_LIMIT),
        cost_estimate=pl.CostEstimate(flops=7 * 3 * 2 * order * order * size, bytes_accessed=1 << 25, transcendentals=0),
    )(ids, prev_square, *g_groups, *d_groups)
    outputs = pl.pallas_call(
        output_kernel, out_shape=[jax.ShapeDtypeStruct((local_rows, local_cols), f32)] * 2,
        in_specs=[SMEM, VMEM, VMEM] + [ANY] * (2 * n_col), out_specs=[VMEM] * 2,
        scratch_shapes=[held, pltpu.SemaphoreType.DMA((2 * n_col,))],
        compiler_params=pltpu.CompilerParams(vmem_limit_bytes=VMEM_LIMIT),
        cost_estimate=pl.CostEstimate(flops=10**9, bytes_accessed=1 << 24, transcendentals=0),
    )
    grad, direction = outputs(ids, beta, dir_prev, *g_groups)

    *exp_own, chosen_z = lax.optimization_barrier((*exp_own, chosen_z))
    chosen_set = (terms[4], send(terms[4], core), chosen_z, send(chosen_z, core))
    exp_in = [send(exp_own[0], over_b(1)), send(exp_own[1], over_b(2)), send(exp_own[2], flip_z(2))]

    trial = pl.pallas_call(
        trial_kernel, out_shape=jax.ShapeDtypeStruct((2, size), f32),
        in_specs=[SMEM, VMEM, VMEM, VMEM] + [ANY] * 4, out_specs=VMEM,
        scratch_shapes=[pltpu.VMEM((order, size), f32), pltpu.VMEM((order, size), jnp.bfloat16),
                        pltpu.VMEM((order, size), jnp.bfloat16),
                        pltpu.VMEM((3, 5, size, size), f32), pltpu.SemaphoreType.DMA((3,))],
        compiler_params=pltpu.CompilerParams(vmem_limit_bytes=VMEM_LIMIT // 2),
        cost_estimate=pl.CostEstimate(flops=3 * 2 * order * order * size, bytes_accessed=1 << 24, transcendentals=0),
    )
    t_own = trial(ids, *exp_own, *chosen_set)
    *exp_in, grad, direction = lax.optimization_barrier((*exp_in, grad, direction))
    t_in = trial(ids, *exp_in, *chosen_set)

    def ordered(bit, mine, theirs):
        return jnp.where(bit == 0, jnp.stack([mine, theirs]), jnp.stack([theirs, mine]))

    t = ordered(half_id, t_own, t_in)
    over = [send(t, flip_z(k)) for k in (2, 1, 3)]
    t = ordered(z % 2, t + over[0], over[1] + over[2])
    t = ordered(r, t, send(t, core))
    t = jnp.transpose(t, (3, 1, 2, 0, 4)).reshape(2, order)
    t = jnp.concatenate([t, jnp.full((1, order), spread_own)], axis=0)
    every = [t] + [send(t, over_b(k)) for k in range(1, n_b)]
    trial_diag, sums = pl.pallas_call(
        closing_kernel, out_shape=[jax.ShapeDtypeStruct((n_b, 2, order), f32), jax.ShapeDtypeStruct((2,), f32)],
        in_specs=[SMEM, SMEM] + [VMEM] * n_b, out_specs=[VMEM, SMEM],
    )(ids, weight_all, *every)
    return (sums[0], sums[1], grad, direction, trial_diag)


def product(left, right):
    return jnp.dot(left, right, precision=HIGHEST, preferred_element_type=jnp.float32)


def shards(m_matrices, bvec_index, weight_table, grad_prev, dir_prev):
    per_group = m_matrices.shape[0]
    local_rows = m_matrices.shape[2]
    local_cols = m_matrices.shape[3]
    matrix_order = local_rows * lax.axis_size("row")
    group_index = lax.axis_index("bvec")
    row_start = lax.axis_index("row") * local_rows
    col_start = lax.axis_index("col") * local_cols
    weight_all = lookup_weights(bvec_index, weight_table)
    weight_own = lax.dynamic_slice_in_dim(weight_all, group_index * per_group, per_group)
    row_ids = row_start + jnp.arange(local_rows, dtype=jnp.int32)
    col_ids = col_start + jnp.arange(local_cols, dtype=jnp.int32)
    on_diag = (row_ids[:, None] == col_ids[None, :]).astype(jnp.float32)
    own_diag = jnp.sum(m_matrices * on_diag, axis=2)
    share_diag = lax.psum(own_diag, "row")
    diagonal = lax.all_gather(share_diag, "col", axis=2, tiled=True)
    row_diag = lax.dynamic_slice_in_dim(diagonal, row_start, local_rows, 2)
    spread_own = (
        jnp.sum(weight_own[:, None] * (1.0 - diagonal[:, 0] ** 2 - diagonal[:, 1] ** 2))
        / matrix_order
    )
    leader = (lax.axis_index("row") == 0) & (lax.axis_index("col") == 0)
    spread_term = jnp.where(leader, spread_own, 0.0)
    differ = row_diag[:, :, :, None] - share_diag[:, :, None, :]
    weighted = 2.0 * weight_own[:, None, None] * jnp.sum(m_matrices * differ, axis=1)
    grad_part = jnp.sum(weighted, axis=0)
    gradient = lax.psum(grad_part, "bvec")
    counted = jnp.where(group_index == 0, 1.0, 0.0)
    grad_square = counted * jnp.sum(gradient * gradient)
    prev_square = counted * jnp.sum(grad_prev * grad_prev)
    cross_term = counted * jnp.sum(gradient * dir_prev)
    dir_square = counted * jnp.sum(dir_prev * dir_prev)
    totals = lax.psum(
        (spread_term, grad_square, prev_square, cross_term, dir_square), ("bvec", "row", "col")
    )
    spread = totals[0]
    beta_factor = totals[1] / (1.0 + totals[2])
    direction = beta_factor * dir_prev - gradient
    dir_norm = jnp.maximum(
        totals[1] - 2.0 * beta_factor * totals[3] + beta_factor * beta_factor * totals[4], 0.0
    )
    generator = STEP_SCALE * direction / jnp.sqrt(1.0 + dir_norm / matrix_order)
    block_ids = col_start + jnp.arange(local_cols, dtype=jnp.int32)
    eye_block = (row_ids[:, None] == block_ids[None, :]).astype(jnp.float32)
    horner_start = eye_block + generator / TAYLOR
    columns = lax.all_gather(generator, "row", axis=0, tiled=True)

    def accumulate(section):
        return product(section, columns)

    def horner_step(counter, current):
        folded = accumulate(lax.all_gather(current, "col", axis=1, tiled=True))
        divisor = (TAYLOR - 1 - counter).astype(jnp.float32)
        return eye_block + folded / divisor

    expmap = lax.fori_loop(0, TAYLOR - 1, horner_step, horner_start)
    expmap_cols = lax.all_gather(expmap, "row", axis=0, tiled=True)
    section = lax.all_gather(m_matrices, "col", axis=3, tiled=True)
    flattened = section.reshape((-1, section.shape[3]))
    rotated = product(flattened, expmap_cols).reshape(
        jnp.zeros(m_matrices.shape, jnp.float32).shape
    )
    trial_part = jnp.sum(expmap[None, None] * rotated, axis=2)
    trial_share = lax.psum(trial_part, "row")
    trial_group = lax.all_gather(trial_share, "col", axis=2, tiled=True)
    trial_diag = lax.all_gather(trial_group, "bvec", axis=0, tiled=True)
    trial_spread = (
        jnp.sum(weight_all[:, None] * (1.0 - trial_diag[:, 0] ** 2 - trial_diag[:, 1] ** 2))
        / matrix_order
    )
    return (spread, trial_spread, gradient, direction, trial_diag)


def solution(mesh):
    placed = (P("bvec", None, "row", "col"), P(), P(), P("row", "col"), P("row", "col"))
    counts = tuple(mesh.shape[a] for a in AXES)
    special = counts == (4, 2, 4)

    def named(*args):
        return paired(counts, *args)

    return jax.shard_map(
        named if special else shards,
        mesh=mesh,
        in_specs=placed,
        out_specs=(P(), P(), P("row", "col"), P("row", "col"), P()),
        check_vma=False,
    )
```

```python
import jax
import jax.numpy as jnp
from jax import lax
from jax.experimental import pallas as pl
from jax.experimental.pallas import tpu as pltpu
from jax.sharding import PartitionSpec as P


TAYLOR = 8
STEP_SCALE = 1.75
HIGHEST = lax.Precision.HIGHEST
AXES = ("bvec", "row", "col")
ANY = pl.BlockSpec(memory_space=pl.ANY)
SMEM = pl.BlockSpec(memory_space=pltpu.SMEM)
VMEM = pl.BlockSpec(memory_space=pltpu.VMEM)
MIB = 1024 * 1024
VMEM_LIMIT = 62 * MIB


def split_bf16(x):
    high = x.astype(jnp.bfloat16)
    low = (x - high.astype(jnp.float32)).astype(jnp.bfloat16)
    return high, low


def dot(a, b):
    return jnp.dot(a, b, preferred_element_type=jnp.float32)


def above(n):
    return lax.broadcasted_iota(jnp.int32, (n, n), 1) > lax.broadcasted_iota(jnp.int32, (n, n), 0)


def pack_block(part, o, value, low_half):
    n = value.shape[0] // 2

    def put(i, rows):
        part[i // 2, i % 2 * n:(i % 2 + 1) * n, :] = rows

    if o == 0:
        mixed = jnp.where(above(n), value[:n, :n], value[n:, n:])
        put(0, jnp.concatenate([mixed, value[:n, n:]], axis=1))
    elif o == 4:
        put(7, jnp.where(low_half, value[:n, :], value[:, n:].T))
    else:
        put(2 * o - 1, value[:n])
        put(2 * o, value[n:])


def unpack_diagonal(rows):
    n = rows.shape[0]
    mixed, corner = rows[:, :n], rows[:, n:]
    upper = jnp.where(above(n), mixed, 0.0)
    below = lax.broadcasted_iota(jnp.int32, (n, n), 1) < lax.broadcasted_iota(jnp.int32, (n, n), 0)
    lower = jnp.where(below, mixed, 0.0)
    return upper - upper.T, corner, -corner.T, lower - lower.T


def packet_kernel(ids, m, prev, out, square, gprev, sem):
    r, z = ids[1], ids[2]
    n = square.shape[1]
    per_core = m.shape[1] // n
    rows = pl.ds(pl.multiple_of(lax.rem(z, per_core) * n, n), n)
    squares = [pltpu.make_async_copy(m.at[p, rows, :], square.at[p], sem.at[p]) for p in range(2)]
    other = pltpu.make_async_copy(prev, gprev, sem.at[2])
    holder = lax.div(z, per_core) == r
    other.start()

    @pl.when(holder)
    def _():
        for c in squares:
            c.start()
        on_diag = lax.broadcasted_iota(jnp.int32, (n, n), 0) == lax.broadcasted_iota(jnp.int32, (n, n), 1)
        for p, c in enumerate(squares):
            c.wait()
            out[p:p + 1, :] = jnp.sum(jnp.where(on_diag, square[p], 0.0), axis=0, keepdims=True)

    @pl.when(jnp.logical_not(holder))
    def _():
        out[0:2, :] = jnp.zeros((2, n), jnp.float32)

    other.wait()
    g = gprev[...]
    total = jnp.sum(jnp.sum((g * g).reshape(-1, 8, n), axis=0))
    out[2:3, :] = jnp.full((1, n), total, jnp.float32)


def term_kernel(ids, weight, diags, own, other, o0, o1, o2, o3, chosen, mre, mim, part, sem, out_sem, chosen_sem):
    b, r, z = ids[0], ids[1], ids[2]
    size = mre.shape[-1]
    per_core = own.shape[1] // size
    blocks = 2 * per_core
    kept = mre.shape[0]
    per_chip = own.shape[2] // size
    groups = blocks // per_chip
    j = z * per_chip + r
    lanes = pl.ds(pl.multiple_of(r * size, size), size)
    for o in range(kept):
        block = lax.rem(j + o, blocks)
        rows = pl.ds(pl.multiple_of(lax.rem(block, per_core) * size, size), size)
        mine = lax.div(block, per_core) == r
        for ref, cond in ((own, mine), (other, jnp.logical_not(mine))):
            @pl.when(cond)
            def _(ref=ref, o=o, rows=rows):
                pltpu.make_async_copy(ref.at[0, rows, lanes], mre.at[o], sem.at[0, o]).start()
                pltpu.make_async_copy(ref.at[1, rows, lanes], mim.at[o], sem.at[1, o]).start()

    def piece(block, p):
        slot = lax.rem(z - lax.div(block, per_chip) + groups, groups)
        half = lax.rem(block, per_chip)
        row = diags[slot, pl.ds(p, 1), :]
        return jnp.where(half == 0, row[:, :size], row[:, size:])

    factor = 2.0 * weight[b]
    re_own, im_own = piece(j, 0), piece(j, 1)
    low_half = j < blocks // 2
    copies = []
    for o in range(kept):
        block = lax.rem(j + o, blocks)
        re_rows = jnp.broadcast_to(piece(block, 0), (size, size)).T
        im_rows = jnp.broadcast_to(piece(block, 1), (size, size)).T
        pltpu.make_async_copy(own.at[0, pl.ds(0, size), pl.ds(0, size)], mre.at[o], sem.at[0, o]).wait()
        pltpu.make_async_copy(own.at[0, pl.ds(0, size), pl.ds(0, size)], mim.at[o], sem.at[1, o]).wait()
        kept_copies = [pltpu.make_async_copy(buf.at[o], chosen.at[p, o], chosen_sem.at[p, o]) for p, buf in enumerate((mre, mim))]
        for copy in kept_copies:
            copy.start()
        copies += kept_copies
        value = factor * (mre[o] * (re_rows - re_own) + mim[o] * (im_rows - im_own))
        pack_block(part, o, value, low_half)
    for k, out in enumerate((o0, o1, o2, o3)):
        copy = pltpu.make_async_copy(part.at[jnp.bitwise_xor(b, k)], out, out_sem.at[k])
        copy.start()
        copies.append(copy)
    for copy in copies:
        copy.wait()


def quarter_kernel(ids, own, other, out, half, buf, sem):
    r, z, h = ids[1], ids[2], ids[4]
    size = buf.shape[2]
    per_core = own.shape[0] // size
    blocks = 2 * per_core
    per_chip = own.shape[1] // size
    j = z * per_chip + r
    lanes = pl.ds(pl.multiple_of(r * size, size), size)
    for o in range(5):
        block = lax.rem(j + o, blocks)
        rows = pl.ds(pl.multiple_of(lax.rem(block, per_core) * size, size), size)
        mine = lax.div(block, per_core) == r
        for ref, cond in ((own, mine), (other, jnp.logical_not(mine))):
            @pl.when(cond)
            def _(ref=ref, rows=rows, o=o):
                pltpu.make_async_copy(ref.at[rows, lanes], buf.at[o], sem.at[o]).start()
    for o in range(5):
        pltpu.make_async_copy(own.at[pl.ds(0, size), pl.ds(0, size)], buf.at[o], sem.at[o]).wait()
        pack_block(out, o, buf[o], j < blocks // 2)
    half[...] = jnp.where(h == 0, out[0:2], out[2:4])


def group_copies(ids, ins, dst, sem, place):
    r, z = ids[1], ids[2]
    groups = len(ins) // 2
    quarter = ins[0].shape[1]
    out = []
    for i, ref in enumerate(ins):
        s, c = i % groups, i // groups
        j = lax.rem(z - s + groups, groups) * 2 + (r if c == 0 else 1 - r)
        for k in range(4):
            rows = pl.ds(pl.multiple_of(place(s, k) * quarter, quarter), quarter)
            out.append(pltpu.make_async_copy(ref.at[k], dst.at[j, rows], sem.at[i]))
    return out


def terms_place(ids):
    return lambda s, k: jnp.bitwise_xor(ids[0], k)


def shared_place(ids):
    h = ids[4]
    return lambda s, k: k if s == 0 else (2 * h + k if k < 2 else 2 * (1 - h) + k - 2)


def solve_kernel(ids, prev_square, *refs):
    groups = (len(refs) - 11) // 4
    g_in, d_in = refs[:2 * groups], refs[2 * groups:4 * groups]
    beta_out, exp_a, exp_b, exp_c, pg, pd, ahi, alo, hhi, hlo, sem = refs[4 * groups:]
    own_block = ids[3]
    order = ahi.shape[0]
    blocks, _, size = pg.shape

    g_copies = group_copies(ids, g_in, pg, sem.at[0], terms_place(ids))
    d_copies = group_copies(ids, d_in, pd, sem.at[1], shared_place(ids))
    for c in g_copies + d_copies:
        c.start()
    strip = size // 2

    def fold(x):
        return jnp.sum(x.reshape(-1, 8, size), axis=0)

    quarter = g_in[0].shape[1]

    def arrive(which, i):
        for k in range(4):
            at = pl.ds(k * quarter, quarter)
            pltpu.make_async_copy(g_in[0].at[k], pg.at[0, at], sem.at[which, i]).wait()
        core = lax.div(i, groups)
        column = lax.rem(ids[2] - lax.rem(i, groups) + groups, groups) * 2
        return column + jnp.where(core == 0, ids[1], 1 - ids[1])

    def norm_body(i, acc):
        jj = arrive(0, i)
        for t in range(0, pg.shape[1], size):
            v = pg[jj, t:t + size, :]
            acc = acc + fold(v * v)
        return acc

    zero = jnp.zeros((8, size), jnp.float32)
    beta = 2.0 * jnp.sum(lax.fori_loop(0, blocks, norm_body, zero)) / (1.0 + prev_square[0])
    beta_out[...] = jnp.full(beta_out.shape, beta, jnp.float32)

    def store(row, col, v):
        high, low = split_bf16(v)
        rows = pl.ds(pl.multiple_of(row, strip), v.shape[0])
        cols = pl.ds(pl.multiple_of(col, strip), v.shape[1])
        ahi[rows, cols] = high
        alo[rows, cols] = low

    def dir_body(i, acc):
        jj = arrive(1, i)
        base = jj * size
        for t in range(8):
            at = slice(t * strip, (t + 1) * strip)
            v = beta * pd[jj, at, :] - pg[jj, at, :]
            acc = acc + fold(v * v)
            if t == 0:
                first_q, second_q, third_q, fourth_q = unpack_diagonal(v)
                store(base, base, first_q)
                store(base, base + strip, second_q)
                store(base + strip, base, third_q)
                store(base + strip, base + strip, fourth_q)
            elif t == 7:
                low_half = jj < blocks // 2
                v = jnp.where(low_half, v, -v)
                high_block = jnp.where(low_half, jj + blocks // 2, jj) * size + jnp.where(low_half, 0, strip)
                low_block = jnp.where(low_half, jj, jj - blocks // 2) * size
                store(high_block, low_block, v)
                store(low_block, high_block, -v.T)
            else:
                row = lax.rem(jj + (t + 1) // 2, blocks) * size + (t + 1) % 2 * strip
                store(row, base, v)
                store(base, row, -v.T)
        return acc

    dir_square = 2.0 * jnp.sum(lax.fori_loop(0, blocks, dir_body, zero))
    scale = STEP_SCALE / jnp.sqrt(jnp.full((1, size), 1.0 + dir_square / order, jnp.float32))

    tile = min(1024, order)
    own_cols = pl.ds(pl.multiple_of(own_block * size, size), size)

    def eye_rows(start, count):
        rid = lax.broadcasted_iota(jnp.int32, (count, size), 0) + start
        cid = lax.broadcasted_iota(jnp.int32, (count, size), 1) + own_block * size
        return (rid == cid).astype(jnp.float32)

    def first(i, carry):
        start = pl.multiple_of(i * size, size)
        rows = pl.ds(start, size)
        a = ahi[rows, own_cols].astype(jnp.float32) + alo[rows, own_cols].astype(jnp.float32)
        high, low = split_bf16(eye_rows(start, size) + a * (scale / TAYLOR))
        hhi[0, rows, :] = high
        hlo[0, rows, :] = low
        return carry

    lax.fori_loop(0, order // size, first, 0)

    def step(counter, carry):
        now = lax.rem(counter, 2)
        divisor = (TAYLOR - 1 - counter).astype(jnp.float32)
        inverse = scale / jnp.full((1, size), divisor, jnp.float32)
        bh = hhi[now]
        bl = hlo[now]

        def rows_body(i, c):
            start = pl.multiple_of(i * tile, tile)
            rows = pl.ds(start, tile)
            ah, al = ahi[rows, :], alo[rows, :]
            value = eye_rows(start, tile) + (dot(ah, bh) + dot(ah, bl) + dot(al, bh)) * inverse

            @pl.when(counter < TAYLOR - 2)
            def _():
                high, low = split_bf16(value)
                hhi[1 - now, rows, :] = high
                hlo[1 - now, rows, :] = low

            for t in range(order // tile):
                @pl.when((counter == TAYLOR - 2) & (i == t))
                def _(t=t):
                    begin = 0
                    for ref in (exp_a, exp_b, exp_c):
                        end = begin + ref.shape[0]
                        lo, hi = max(begin, t * tile), min(end, (t + 1) * tile)
                        if lo < hi:
                            ref[lo - begin:hi - begin, :] = value[lo - t * tile:hi - t * tile]
                        begin = end
            return c

        return lax.fori_loop(0, order // tile, rows_body, carry)

    lax.fori_loop(0, TAYLOR - 1, step, 0)


def output_kernel(ids, beta, dprev, *refs):
    g_in = refs[:-4]
    grad_out, dir_out, pg, sem = refs[-4:]
    r, z = ids[1], ids[2]
    blocks, _, size = pg.shape
    per_core = grad_out.shape[0] // size
    per_chip = grad_out.shape[1] // size
    for c in group_copies(ids, g_in, pg, sem, terms_place(ids)):
        c.start()
    for c in group_copies(ids, g_in, pg, sem, terms_place(ids)):
        c.wait()

    def out_body(t, carry):
        i, jx = lax.div(t, per_chip), lax.rem(t, per_chip)
        rb, cb = r * per_core + i, z * per_chip + jx
        o = lax.rem(rb - cb + blocks, blocks)
        rows = pl.ds(pl.multiple_of(i * size, size), size)
        cols = pl.ds(pl.multiple_of(jx * size, size), size)

        n = size // 2

        @pl.when(o == 0)
        def _():
            first_q, second_q, third_q, fourth_q = unpack_diagonal(pg[cb, :n, :])
            grad_out[rows, cols] = jnp.concatenate(
                [jnp.concatenate([first_q, second_q], axis=1), jnp.concatenate([third_q, fourth_q], axis=1)], axis=0)

        @pl.when((o > 0) & (o < 4))
        def _():
            grad_out[rows, cols] = pg[cb, pl.ds(pl.multiple_of(o * size - n, n), size), :]

        @pl.when(o > 4)
        def _():
            grad_out[rows, cols] = -pg[rb, pl.ds(pl.multiple_of((blocks - o) * size - n, n), size), :].T

        @pl.when((o == 4) & (rb > cb))
        def _():
            grad_out[rows, cols] = jnp.concatenate([pg[cb, 7 * n:, :], -pg[rb, 7 * n:, :]], axis=0)

        @pl.when((o == 4) & (rb < cb))
        def _():
            grad_out[rows, cols] = jnp.concatenate([-pg[rb, 7 * n:, :], pg[cb, 7 * n:, :]], axis=0).T

        dir_out[rows, cols] = beta[0:1, 0:1] * dprev[rows, cols] - grad_out[rows, cols]
        return carry

    lax.fori_loop(0, per_core * per_chip, out_body, 0)


def trial_kernel(ids, exp_a, exp_b, exp_c, m0, m1, m2, m3, out, e, ehi, elo, mbuf, sem):
    r, z = ids[1], ids[2]
    width = exp_a.shape[1]
    size = m0.shape[2]
    blocks = e.shape[0] // size
    work = [(i, p) for i in range(4) for p in range(2)]
    sources = (m0, m1, m2, m3)

    def copy(n):
        i, p = work[n]
        return pltpu.make_async_copy(sources[i].at[p], mbuf.at[n % 3], sem.at[n % 3])

    copy(0).start()
    copy(1).start()
    begin = 0
    for ref in (exp_a, exp_b, exp_c):
        high, low = split_bf16(ref[...])
        rows = slice(begin, begin + ref.shape[0])
        e[rows, :] = ref[...]
        ehi[rows, :] = high
        elo[rows, :] = low
        begin += ref.shape[0]
    totals = [jnp.zeros((8, width), jnp.float32) for _ in range(2)]
    for n, (i, p) in enumerate(work):
        if n + 2 < len(work):
            copy(n + 2).start()
        copy(n).wait()
        chip = z if i < 2 else jnp.bitwise_xor(z, 1)
        j = chip * 2 + (r if i % 2 == 0 else 1 - r)
        own = pl.ds(pl.multiple_of(j * size, size), size)
        bh, bl = ehi[own, :], elo[own, :]
        for o in range(5):
            high, low = split_bf16(mbuf[n % 3, o])
            value = dot(high, bh) + dot(high, bl) + dot(low, bh)
            at = pl.ds(pl.multiple_of(lax.rem(j + o, blocks) * size, size), size)
            term = jnp.sum((e[at, :] * value).reshape(-1, 8, width), axis=0)
            totals[p] = totals[p] + (term if o in (0, 4) else 2.0 * term)
    out[...] = jnp.concatenate([jnp.sum(t, axis=0, keepdims=True) for t in totals], axis=0)


def closing_kernel(ids, weights, *refs):
    diag_out, spread_out, trial_out = refs[-3:]
    order = diag_out.shape[2]
    spread, trial = jnp.float32(0.0), jnp.float32(0.0)
    for k, ref in enumerate(refs[:-3]):
        group = jnp.bitwise_xor(ids[0], k)
        re, im = ref[0:1, :], ref[1:2, :]
        diag_out[group] = ref[0:2, :]
        spread = spread + ref[2, 0]
        trial = trial + weights[group] * jnp.sum(1.0 - re * re - im * im)
    spread_out[0] = spread
    trial_out[0] = trial / order


def lookup_weights(bvec_index, weight_table):
    table_slots = jnp.arange(weight_table.shape[0], dtype=jnp.int32)
    return jnp.sum(
        jnp.where(table_slots[None, :] == bvec_index[:, None], weight_table[None, :], 0.0), axis=1
    )


def paired(counts, m_matrices, bvec_index, weight_table, grad_prev, dir_prev):
    n_b, n_row, n_col = counts
    local_rows, local_cols = m_matrices.shape[2], m_matrices.shape[3]
    order = local_rows * n_row
    size = local_cols // n_row
    b, r, z = (lax.axis_index(a).astype(jnp.int32) for a in AXES)
    parity = jnp.bitwise_xor(b, b >> 1) & 1
    half_id = jnp.bitwise_xor(parity, z >> 1) & 1
    own_block = (z % 2) * 4 + half_id * 2 + r
    ids = jnp.stack([b, r, z, own_block, parity]).astype(jnp.int32)

    def send(x, where):
        pairs = []
        for bb in range(n_b):
            for rr in range(n_row):
                for zz in range(n_col):
                    tb, tr, tz = where(bb, rr, zz)
                    pairs.append(((bb * n_row + rr) * n_col + zz, (tb * n_row + tr) * n_col + tz))
        return lax.ppermute(x, AXES, pairs)

    core = lambda bb, rr, zz: (bb, 1 - rr, zz)
    over_b = lambda k: (lambda bb, rr, zz: (bb ^ k, rr, zz))
    over_z = lambda s: (lambda bb, rr, zz: (bb, rr, (zz + s) % n_col))
    flip_z = lambda k: (lambda bb, rr, zz: (bb, rr, zz ^ k))

    weight_all = lookup_weights(bvec_index, weight_table)
    weight_own = lax.dynamic_slice_in_dim(weight_all, b, 1)
    m = m_matrices[0]

    d_oth = send(dir_prev, core)
    packet = pl.pallas_call(
        packet_kernel, out_shape=jax.ShapeDtypeStruct((3, local_cols), jnp.float32),
        in_specs=[SMEM, ANY, ANY], out_specs=VMEM,
        scratch_shapes=[pltpu.VMEM((2, local_cols, local_cols), jnp.float32), pltpu.VMEM(grad_prev.shape, jnp.float32),
                        pltpu.SemaphoreType.DMA((3,))],
        compiler_params=pltpu.CompilerParams(vmem_limit_bytes=8 * MIB),
        cost_estimate=pl.CostEstimate(flops=10**6, bytes_accessed=1 << 22, transcendentals=0),
    )(ids, m, grad_prev)
    packet = packet + send(packet, core)
    m_oth = send(m, core)
    d_own, d_half = pl.pallas_call(
        quarter_kernel, out_shape=[jax.ShapeDtypeStruct((n, size, size), jnp.float32) for n in (4, 2)],
        in_specs=[SMEM, ANY, ANY], out_specs=[VMEM] * 2,
        scratch_shapes=[pltpu.VMEM((5, size, size), jnp.float32), pltpu.SemaphoreType.DMA((5,))],
        compiler_params=pltpu.CompilerParams(vmem_limit_bytes=8 * MIB),
        cost_estimate=pl.CostEstimate(flops=0, bytes_accessed=1 << 20, transcendentals=0),
    )(ids, dir_prev, d_oth)
    packet, d_half = lax.optimization_barrier((packet, d_half))
    diags = jnp.stack([packet] + [send(packet, over_z(s)) for s in range(1, n_col)])
    prev_square = jnp.sum(diags[:, 2, :1], axis=0)
    spread_own = weight_own[0] * jnp.sum(1.0 - diags[:, 0] ** 2 - diags[:, 1] ** 2) / order

    quarter = jax.ShapeDtypeStruct((size, size), jnp.float32)
    d_by_z = {s: send(d_half, over_z(s)) for s in (1, 3, 2)}
    terms = pl.pallas_call(
        term_kernel, out_shape=[quarter] * 4 + [jax.ShapeDtypeStruct((2, 5, size, size), jnp.float32)],
        in_specs=[SMEM, SMEM, VMEM, ANY, ANY], out_specs=[ANY] * 5,
        scratch_shapes=[pltpu.VMEM((5, size, size), jnp.float32), pltpu.VMEM((5, size, size), jnp.float32),
                        pltpu.VMEM((4, size, size), jnp.float32),
                        pltpu.SemaphoreType.DMA((2, 5)), pltpu.SemaphoreType.DMA((4,)),
                        pltpu.SemaphoreType.DMA((2, 5))],
        compiler_params=pltpu.CompilerParams(vmem_limit_bytes=12 * MIB),
        cost_estimate=pl.CostEstimate(flops=10**9, bytes_accessed=1 << 22, transcendentals=0),
    )(ids, weight_all, diags, m, m_oth)
    parts = [send(terms[k], over_b(k)) for k in range(1, n_b)]
    g_quarter = ((terms[0] + parts[0]) + parts[1]) + parts[2]

    d_groups = [d_own] + [
        jnp.concatenate([d_by_z[s], send(d_by_z[s][:1], over_b(1)), send(d_by_z[s][1:], over_b(2))])
        for s in range(1, n_col)
    ]
    d_groups = d_groups + [send(g, core) for g in d_groups]
    g_by_z = {0: g_quarter}
    for s in (1, 3, 2):
        g_by_z[s] = send(g_quarter, over_z(s))
    g_groups = []
    for s in range(n_col):
        piece = g_by_z[s]
        over_x = send(piece, over_b(1))
        over_y = send(piece, over_b(2))
        if s in (1, 2):
            across = send(over_y, over_b(1))
        else:
            across = send(over_x, over_b(2))
        g_groups.append(jnp.stack([piece, over_x, over_y, across]))
    g_groups = g_groups + [send(g, core) for g in g_groups]
    chosen_z = send(terms[4], flip_z(1))

    f32 = jnp.float32
    held = pltpu.VMEM((2 * n_col, 4 * size, size), f32)
    by_plane = 13 * order // 32 // 8 * 8
    shares = (by_plane, by_plane, order - 2 * by_plane)
    beta, *exp_own = pl.pallas_call(
        solve_kernel,
        out_shape=[jax.ShapeDtypeStruct((8, 128), f32)] + [jax.ShapeDtypeStruct((n, size), f32) for n in shares],
        in_specs=[SMEM, SMEM] + [ANY] * (4 * n_col), out_specs=[VMEM] * 4,
        scratch_shapes=[held, held,
                        pltpu.VMEM((order, order), jnp.bfloat16), pltpu.VMEM((order, order), jnp.bfloat16),
                        pltpu.VMEM((2, order, size), jnp.bfloat16), pltpu.VMEM((2, order, size), jnp.bfloat16),
                        pltpu.SemaphoreType.DMA((2, 2 * n_col))],
        compiler_params=pltpu.CompilerParams(vmem_limit_bytes=46 * MIB),
        cost_estimate=pl.CostEstimate(flops=7 * 3 * 2 * order * order * size, bytes_accessed=1 << 25, transcendentals=0),
    )(ids, prev_square, *g_groups, *d_groups)
    outputs = pl.pallas_call(
        output_kernel, out_shape=[jax.ShapeDtypeStruct((local_rows, local_cols), f32)] * 2,
        in_specs=[SMEM, VMEM, VMEM] + [ANY] * (2 * n_col), out_specs=[VMEM] * 2,
        scratch_shapes=[held, pltpu.SemaphoreType.DMA((2 * n_col,))],
        compiler_params=pltpu.CompilerParams(vmem_limit_bytes=VMEM_LIMIT),
        cost_estimate=pl.CostEstimate(flops=10**9, bytes_accessed=1 << 24, transcendentals=0),
    )
    grad, direction = outputs(ids, beta, dir_prev, *g_groups)

    *exp_own, chosen_z = lax.optimization_barrier((*exp_own, chosen_z))
    chosen_set = (terms[4], send(terms[4], core), chosen_z, send(chosen_z, core))
    exp_in = [send(exp_own[0], over_b(1)), send(exp_own[1], over_b(2)), send(exp_own[2], flip_z(2))]

    trial = pl.pallas_call(
        trial_kernel, out_shape=jax.ShapeDtypeStruct((2, size), f32),
        in_specs=[SMEM, VMEM, VMEM, VMEM] + [ANY] * 4, out_specs=VMEM,
        scratch_shapes=[pltpu.VMEM((order, size), f32), pltpu.VMEM((order, size), jnp.bfloat16),
                        pltpu.VMEM((order, size), jnp.bfloat16),
                        pltpu.VMEM((3, 5, size, size), f32), pltpu.SemaphoreType.DMA((3,))],
        compiler_params=pltpu.CompilerParams(vmem_limit_bytes=20 * MIB),
        cost_estimate=pl.CostEstimate(flops=3 * 2 * order * order * size, bytes_accessed=1 << 24, transcendentals=0),
    )
    t_own = trial(ids, *exp_own, *chosen_set)
    *exp_in, grad, direction = lax.optimization_barrier((*exp_in, grad, direction))
    t_in = trial(ids, *exp_in, *chosen_set)

    def ordered(bit, mine, theirs):
        return jnp.where(bit == 0, jnp.stack([mine, theirs]), jnp.stack([theirs, mine]))

    t = ordered(half_id, t_own, t_in)
    over = [send(t, flip_z(k)) for k in (2, 1, 3)]
    t = ordered(z % 2, t + over[0], over[1] + over[2])
    t = ordered(r, t, send(t, core))
    t = jnp.transpose(t, (3, 1, 2, 0, 4)).reshape(2, order)
    t = jnp.concatenate([t, jnp.full((1, order), spread_own)], axis=0)
    every = [t] + [send(t, over_b(k)) for k in range(1, n_b)]
    one = jax.ShapeDtypeStruct((1,), f32)
    trial_diag, spread, trial_spread = pl.pallas_call(
        closing_kernel, out_shape=[jax.ShapeDtypeStruct((n_b, 2, order), f32), one, one],
        in_specs=[SMEM, SMEM] + [VMEM] * n_b, out_specs=[VMEM, SMEM, SMEM],
        compiler_params=pltpu.CompilerParams(vmem_limit_bytes=4 * MIB),
    )(ids, weight_all, *every)
    return (spread.reshape(()), trial_spread.reshape(()), grad, direction, trial_diag)


def product(left, right):
    return jnp.dot(left, right, precision=HIGHEST, preferred_element_type=jnp.float32)


def shards(m_matrices, bvec_index, weight_table, grad_prev, dir_prev):
    per_group = m_matrices.shape[0]
    local_rows = m_matrices.shape[2]
    local_cols = m_matrices.shape[3]
    matrix_order = local_rows * lax.axis_size("row")
    group_index = lax.axis_index("bvec")
    row_start = lax.axis_index("row") * local_rows
    col_start = lax.axis_index("col") * local_cols
    weight_all = lookup_weights(bvec_index, weight_table)
    weight_own = lax.dynamic_slice_in_dim(weight_all, group_index * per_group, per_group)
    row_ids = row_start + jnp.arange(local_rows, dtype=jnp.int32)
    col_ids = col_start + jnp.arange(local_cols, dtype=jnp.int32)
    on_diag = (row_ids[:, None] == col_ids[None, :]).astype(jnp.float32)
    own_diag = jnp.sum(m_matrices * on_diag, axis=2)
    share_diag = lax.psum(own_diag, "row")
    diagonal = lax.all_gather(share_diag, "col", axis=2, tiled=True)
    row_diag = lax.dynamic_slice_in_dim(diagonal, row_start, local_rows, 2)
    spread_own = (
        jnp.sum(weight_own[:, None] * (1.0 - diagonal[:, 0] ** 2 - diagonal[:, 1] ** 2))
        / matrix_order
    )
    leader = (lax.axis_index("row") == 0) & (lax.axis_index("col") == 0)
    spread_term = jnp.where(leader, spread_own, 0.0)
    differ = row_diag[:, :, :, None] - share_diag[:, :, None, :]
    weighted = 2.0 * weight_own[:, None, None] * jnp.sum(m_matrices * differ, axis=1)
    grad_part = jnp.sum(weighted, axis=0)
    gradient = lax.psum(grad_part, "bvec")
    counted = jnp.where(group_index == 0, 1.0, 0.0)
    grad_square = counted * jnp.sum(gradient * gradient)
    prev_square = counted * jnp.sum(grad_prev * grad_prev)
    cross_term = counted * jnp.sum(gradient * dir_prev)
    dir_square = counted * jnp.sum(dir_prev * dir_prev)
    totals = lax.psum(
        (spread_term, grad_square, prev_square, cross_term, dir_square), ("bvec", "row", "col")
    )
    spread = totals[0]
    beta_factor = totals[1] / (1.0 + totals[2])
    direction = beta_factor * dir_prev - gradient
    dir_norm = jnp.maximum(
        totals[1] - 2.0 * beta_factor * totals[3] + beta_factor * beta_factor * totals[4], 0.0
    )
    generator = STEP_SCALE * direction / jnp.sqrt(1.0 + dir_norm / matrix_order)
    block_ids = col_start + jnp.arange(local_cols, dtype=jnp.int32)
    eye_block = (row_ids[:, None] == block_ids[None, :]).astype(jnp.float32)
    horner_start = eye_block + generator / TAYLOR
    columns = lax.all_gather(generator, "row", axis=0, tiled=True)

    def accumulate(section):
        return product(section, columns)

    def horner_step(counter, current):
        folded = accumulate(lax.all_gather(current, "col", axis=1, tiled=True))
        divisor = (TAYLOR - 1 - counter).astype(jnp.float32)
        return eye_block + folded / divisor

    expmap = lax.fori_loop(0, TAYLOR - 1, horner_step, horner_start)
    expmap_cols = lax.all_gather(expmap, "row", axis=0, tiled=True)
    section = lax.all_gather(m_matrices, "col", axis=3, tiled=True)
    flattened = section.reshape((-1, section.shape[3]))
    rotated = product(flattened, expmap_cols).reshape(
        jnp.zeros(m_matrices.shape, jnp.float32).shape
    )
    trial_part = jnp.sum(expmap[None, None] * rotated, axis=2)
    trial_share = lax.psum(trial_part, "row")
    trial_group = lax.all_gather(trial_share, "col", axis=2, tiled=True)
    trial_diag = lax.all_gather(trial_group, "bvec", axis=0, tiled=True)
    trial_spread = (
        jnp.sum(weight_all[:, None] * (1.0 - trial_diag[:, 0] ** 2 - trial_diag[:, 1] ** 2))
        / matrix_order
    )
    return (spread, trial_spread, gradient, direction, trial_diag)


def solution(mesh):
    placed = (P("bvec", None, "row", "col"), P(), P(), P("row", "col"), P("row", "col"))
    counts = tuple(mesh.shape[a] for a in AXES)
    special = counts == (4, 2, 4)

    def named(*args):
        return paired(counts, *args)

    return jax.shard_map(
        named if special else shards,
        mesh=mesh,
        in_specs=placed,
        out_specs=(P(), P(), P("row", "col"), P("row", "col"), P()),
        check_vma=False,
    )
```

```python
import jax
import jax.numpy as jnp
from jax import lax
from jax.experimental import pallas as pl
from jax.experimental.pallas import tpu as pltpu
from jax.sharding import PartitionSpec as P


TAYLOR = 8
STEP_SCALE = 1.75
HIGHEST = lax.Precision.HIGHEST
AXES = ("bvec", "row", "col")
ANY = pl.BlockSpec(memory_space=pl.ANY)
SMEM = pl.BlockSpec(memory_space=pltpu.SMEM)
VMEM = pl.BlockSpec(memory_space=pltpu.VMEM)
MIB = 1024 * 1024
VMEM_LIMIT = 62 * MIB


def split_bf16(x):
    high = x.astype(jnp.bfloat16)
    low = (x - high.astype(jnp.float32)).astype(jnp.bfloat16)
    return high, low


def dot(a, b):
    return jnp.dot(a, b, preferred_element_type=jnp.float32)


def above(n):
    return lax.broadcasted_iota(jnp.int32, (n, n), 1) > lax.broadcasted_iota(jnp.int32, (n, n), 0)


def pack_block(part, o, value, low_half):
    n = value.shape[0] // 2

    def put(i, rows):
        part[i // 2, i % 2 * n:(i % 2 + 1) * n, :] = rows

    if o == 0:
        mixed = jnp.where(above(n), value[:n, :n], value[n:, n:])
        put(0, jnp.concatenate([mixed, value[:n, n:]], axis=1))
    elif o == 4:
        put(7, jnp.where(low_half, value[:n, :], value[:, n:].T))
    else:
        put(2 * o - 1, value[:n])
        put(2 * o, value[n:])


def unpack_diagonal(rows):
    n = rows.shape[0]
    mixed, corner = rows[:, :n], rows[:, n:]
    upper = jnp.where(above(n), mixed, 0.0)
    below = lax.broadcasted_iota(jnp.int32, (n, n), 1) < lax.broadcasted_iota(jnp.int32, (n, n), 0)
    lower = jnp.where(below, mixed, 0.0)
    return upper - upper.T, corner, -corner.T, lower - lower.T


def packet_kernel(ids, m, prev, out, square, gprev, sem):
    r, z = ids[1], ids[2]
    n = square.shape[1]
    per_core = m.shape[1] // n
    rows = pl.ds(pl.multiple_of(lax.rem(z, per_core) * n, n), n)
    squares = [pltpu.make_async_copy(m.at[p, rows, :], square.at[p], sem.at[p]) for p in range(2)]
    other = pltpu.make_async_copy(prev, gprev, sem.at[2])
    holder = lax.div(z, per_core) == r
    other.start()

    @pl.when(holder)
    def _():
        for c in squares:
            c.start()
        on_diag = lax.broadcasted_iota(jnp.int32, (n, n), 0) == lax.broadcasted_iota(jnp.int32, (n, n), 1)
        for p, c in enumerate(squares):
            c.wait()
            out[p:p + 1, :] = jnp.sum(jnp.where(on_diag, square[p], 0.0), axis=0, keepdims=True)

    @pl.when(jnp.logical_not(holder))
    def _():
        out[0:2, :] = jnp.zeros((2, n), jnp.float32)

    other.wait()
    g = gprev[...]
    total = jnp.sum(jnp.sum((g * g).reshape(-1, 8, n), axis=0))
    out[2:3, :] = jnp.full((1, n), total, jnp.float32)


def term_kernel(ids, weight, diags, own, other, o0, o1, o2, o3, chosen, mre, mim, part, sem, out_sem, chosen_sem):
    b, r, z = ids[0], ids[1], ids[2]
    size = mre.shape[-1]
    per_core = own.shape[1] // size
    blocks = 2 * per_core
    kept = mre.shape[0]
    per_chip = own.shape[2] // size
    groups = blocks // per_chip
    j = z * per_chip + r
    lanes = pl.ds(pl.multiple_of(r * size, size), size)
    for o in range(kept):
        block = lax.rem(j + o, blocks)
        rows = pl.ds(pl.multiple_of(lax.rem(block, per_core) * size, size), size)
        mine = lax.div(block, per_core) == r
        for ref, cond in ((own, mine), (other, jnp.logical_not(mine))):
            @pl.when(cond)
            def _(ref=ref, o=o, rows=rows):
                pltpu.make_async_copy(ref.at[0, rows, lanes], mre.at[o], sem.at[0, o]).start()
                pltpu.make_async_copy(ref.at[1, rows, lanes], mim.at[o], sem.at[1, o]).start()

    def piece(block, p):
        slot = lax.rem(z - lax.div(block, per_chip) + groups, groups)
        half = lax.rem(block, per_chip)
        row = diags[slot, pl.ds(p, 1), :]
        return jnp.where(half == 0, row[:, :size], row[:, size:])

    factor = 2.0 * weight[b]
    re_own, im_own = piece(j, 0), piece(j, 1)
    low_half = j < blocks // 2
    copies = []
    for o in range(kept):
        block = lax.rem(j + o, blocks)
        re_rows = jnp.broadcast_to(piece(block, 0), (size, size)).T
        im_rows = jnp.broadcast_to(piece(block, 1), (size, size)).T
        pltpu.make_async_copy(own.at[0, pl.ds(0, size), pl.ds(0, size)], mre.at[o], sem.at[0, o]).wait()
        pltpu.make_async_copy(own.at[0, pl.ds(0, size), pl.ds(0, size)], mim.at[o], sem.at[1, o]).wait()
        kept_copies = [pltpu.make_async_copy(buf.at[o], chosen.at[p, o], chosen_sem.at[p, o]) for p, buf in enumerate((mre, mim))]
        for copy in kept_copies:
            copy.start()
        copies += kept_copies
        value = factor * (mre[o] * (re_rows - re_own) + mim[o] * (im_rows - im_own))
        pack_block(part, o, value, low_half)
    for k, out in enumerate((o0, o1, o2, o3)):
        copy = pltpu.make_async_copy(part.at[jnp.bitwise_xor(b, k)], out, out_sem.at[k])
        copy.start()
        copies.append(copy)
    for copy in copies:
        copy.wait()


def quarter_kernel(ids, own, other, out, half, buf, sem):
    r, z, h = ids[1], ids[2], ids[4]
    size = buf.shape[2]
    per_core = own.shape[0] // size
    blocks = 2 * per_core
    per_chip = own.shape[1] // size
    j = z * per_chip + r
    lanes = pl.ds(pl.multiple_of(r * size, size), size)
    for o in range(5):
        block = lax.rem(j + o, blocks)
        rows = pl.ds(pl.multiple_of(lax.rem(block, per_core) * size, size), size)
        mine = lax.div(block, per_core) == r
        for ref, cond in ((own, mine), (other, jnp.logical_not(mine))):
            @pl.when(cond)
            def _(ref=ref, rows=rows, o=o):
                pltpu.make_async_copy(ref.at[rows, lanes], buf.at[o], sem.at[o]).start()
    for o in range(5):
        pltpu.make_async_copy(own.at[pl.ds(0, size), pl.ds(0, size)], buf.at[o], sem.at[o]).wait()
        pack_block(out, o, buf[o], j < blocks // 2)
    half[...] = jnp.where(h == 0, out[0:2], out[2:4])


def group_copies(ids, ins, dst, sem, place):
    r, z = ids[1], ids[2]
    groups = len(ins) // 2
    quarter = ins[0].shape[1]
    out = []
    for i, ref in enumerate(ins):
        s, c = i % groups, i // groups
        j = jnp.bitwise_xor(z, s) * 2 + (r if c == 0 else 1 - r)
        for k in range(4):
            rows = pl.ds(pl.multiple_of(place(s, k) * quarter, quarter), quarter)
            out.append(pltpu.make_async_copy(ref.at[k], dst.at[j, rows], sem.at[i]))
    return out


def terms_place(ids):
    return lambda s, k: jnp.bitwise_xor(ids[0], k)


def shared_place(ids):
    h = ids[4]
    return lambda s, k: k if s == 0 else (2 * h + k if k < 2 else 2 * (1 - h) + k - 2)


def solve_kernel(ids, prev_square, *refs):
    groups = (len(refs) - 11) // 4
    g_in, d_in = refs[:2 * groups], refs[2 * groups:4 * groups]
    beta_out, exp_a, exp_b, exp_c, pg, pd, ahi, alo, hhi, hlo, sem = refs[4 * groups:]
    own_block = ids[3]
    order = ahi.shape[0]
    blocks, _, size = pg.shape

    g_copies = group_copies(ids, g_in, pg, sem.at[0], terms_place(ids))
    d_copies = group_copies(ids, d_in, pd, sem.at[1], shared_place(ids))
    for c in g_copies + d_copies:
        c.start()
    strip = size // 2

    def fold(x):
        return jnp.sum(x.reshape(-1, 8, size), axis=0)

    quarter = g_in[0].shape[1]

    def arrive(which, i):
        for k in range(4):
            at = pl.ds(k * quarter, quarter)
            pltpu.make_async_copy(g_in[0].at[k], pg.at[0, at], sem.at[which, i]).wait()
        core = lax.div(i, groups)
        column = jnp.bitwise_xor(ids[2], lax.rem(i, groups)) * 2
        return column + jnp.where(core == 0, ids[1], 1 - ids[1])

    def norm_body(i, acc):
        jj = arrive(0, i)
        for t in range(0, pg.shape[1], size):
            v = pg[jj, t:t + size, :]
            acc = acc + fold(v * v)
        return acc

    zero = jnp.zeros((8, size), jnp.float32)
    beta = 2.0 * jnp.sum(lax.fori_loop(0, blocks, norm_body, zero)) / (1.0 + prev_square[0])
    beta_out[...] = jnp.full(beta_out.shape, beta, jnp.float32)

    def store(row, col, v):
        high, low = split_bf16(v)
        rows = pl.ds(pl.multiple_of(row, strip), v.shape[0])
        cols = pl.ds(pl.multiple_of(col, strip), v.shape[1])
        ahi[rows, cols] = high
        alo[rows, cols] = low

    def dir_body(i, acc):
        jj = arrive(1, i)
        base = jj * size
        for t in range(8):
            at = slice(t * strip, (t + 1) * strip)
            v = beta * pd[jj, at, :] - pg[jj, at, :]
            acc = acc + fold(v * v)
            if t == 0:
                first_q, second_q, third_q, fourth_q = unpack_diagonal(v)
                store(base, base, first_q)
                store(base, base + strip, second_q)
                store(base + strip, base, third_q)
                store(base + strip, base + strip, fourth_q)
            elif t == 7:
                low_half = jj < blocks // 2
                v = jnp.where(low_half, v, -v)
                high_block = jnp.where(low_half, jj + blocks // 2, jj) * size + jnp.where(low_half, 0, strip)
                low_block = jnp.where(low_half, jj, jj - blocks // 2) * size
                store(high_block, low_block, v)
                store(low_block, high_block, -v.T)
            else:
                row = lax.rem(jj + (t + 1) // 2, blocks) * size + (t + 1) % 2 * strip
                store(row, base, v)
                store(base, row, -v.T)
        return acc

    dir_square = 2.0 * jnp.sum(lax.fori_loop(0, blocks, dir_body, zero))
    scale = STEP_SCALE / jnp.sqrt(jnp.full((1, size), 1.0 + dir_square / order, jnp.float32))

    tile = min(1024, order)
    own_cols = pl.ds(pl.multiple_of(own_block * size, size), size)

    def eye_rows(start, count):
        rid = lax.broadcasted_iota(jnp.int32, (count, size), 0) + start
        cid = lax.broadcasted_iota(jnp.int32, (count, size), 1) + own_block * size
        return (rid == cid).astype(jnp.float32)

    def first(i, carry):
        start = pl.multiple_of(i * size, size)
        rows = pl.ds(start, size)
        a = ahi[rows, own_cols].astype(jnp.float32) + alo[rows, own_cols].astype(jnp.float32)
        high, low = split_bf16(eye_rows(start, size) + a * (scale / TAYLOR))
        hhi[0, rows, :] = high
        hlo[0, rows, :] = low
        return carry

    lax.fori_loop(0, order // size, first, 0)

    def step(counter, carry):
        now = lax.rem(counter, 2)
        divisor = (TAYLOR - 1 - counter).astype(jnp.float32)
        inverse = scale / jnp.full((1, size), divisor, jnp.float32)
        bh = hhi[now]
        bl = hlo[now]

        def rows_body(i, c):
            start = pl.multiple_of(i * tile, tile)
            rows = pl.ds(start, tile)
            ah, al = ahi[rows, :], alo[rows, :]
            value = eye_rows(start, tile) + (dot(ah, bh) + dot(ah, bl) + dot(al, bh)) * inverse

            @pl.when(counter < TAYLOR - 2)
            def _():
                high, low = split_bf16(value)
                hhi[1 - now, rows, :] = high
                hlo[1 - now, rows, :] = low

            for t in range(order // tile):
                @pl.when((counter == TAYLOR - 2) & (i == t))
                def _(t=t):
                    begin = 0
                    for ref in (exp_a, exp_b, exp_c):
                        end = begin + ref.shape[0]
                        lo, hi = max(begin, t * tile), min(end, (t + 1) * tile)
                        if lo < hi:
                            ref[lo - begin:hi - begin, :] = value[lo - t * tile:hi - t * tile]
                        begin = end
            return c

        return lax.fori_loop(0, order // tile, rows_body, carry)

    lax.fori_loop(0, TAYLOR - 1, step, 0)


def output_kernel(ids, beta, dprev, *refs):
    g_in = refs[:-4]
    grad_out, dir_out, pg, sem = refs[-4:]
    r, z = ids[1], ids[2]
    blocks, _, size = pg.shape
    per_core = grad_out.shape[0] // size
    per_chip = grad_out.shape[1] // size
    for c in group_copies(ids, g_in, pg, sem, terms_place(ids)):
        c.start()
    for c in group_copies(ids, g_in, pg, sem, terms_place(ids)):
        c.wait()

    def out_body(t, carry):
        i, jx = lax.div(t, per_chip), lax.rem(t, per_chip)
        rb, cb = r * per_core + i, z * per_chip + jx
        o = lax.rem(rb - cb + blocks, blocks)
        rows = pl.ds(pl.multiple_of(i * size, size), size)
        cols = pl.ds(pl.multiple_of(jx * size, size), size)

        n = size // 2

        @pl.when(o == 0)
        def _():
            first_q, second_q, third_q, fourth_q = unpack_diagonal(pg[cb, :n, :])
            grad_out[rows, cols] = jnp.concatenate(
                [jnp.concatenate([first_q, second_q], axis=1), jnp.concatenate([third_q, fourth_q], axis=1)], axis=0)

        @pl.when((o > 0) & (o < 4))
        def _():
            grad_out[rows, cols] = pg[cb, pl.ds(pl.multiple_of(o * size - n, n), size), :]

        @pl.when(o > 4)
        def _():
            grad_out[rows, cols] = -pg[rb, pl.ds(pl.multiple_of((blocks - o) * size - n, n), size), :].T

        @pl.when((o == 4) & (rb > cb))
        def _():
            grad_out[rows, cols] = jnp.concatenate([pg[cb, 7 * n:, :], -pg[rb, 7 * n:, :]], axis=0)

        @pl.when((o == 4) & (rb < cb))
        def _():
            grad_out[rows, cols] = jnp.concatenate([-pg[rb, 7 * n:, :], pg[cb, 7 * n:, :]], axis=0).T

        dir_out[rows, cols] = beta[0:1, 0:1] * dprev[rows, cols] - grad_out[rows, cols]
        return carry

    lax.fori_loop(0, per_core * per_chip, out_body, 0)


def trial_kernel(ids, exp_a, exp_b, exp_c, m0, m1, m2, m3, out, e, ehi, elo, mbuf, sem):
    r, z = ids[1], ids[2]
    width = exp_a.shape[1]
    size = m0.shape[2]
    blocks = e.shape[0] // size
    work = [(i, p) for i in range(4) for p in range(2)]
    sources = (m0, m1, m2, m3)

    def copy(n):
        i, p = work[n]
        return pltpu.make_async_copy(sources[i].at[p], mbuf.at[n % 3], sem.at[n % 3])

    copy(0).start()
    copy(1).start()
    begin = 0
    for ref in (exp_a, exp_b, exp_c):
        high, low = split_bf16(ref[...])
        rows = slice(begin, begin + ref.shape[0])
        e[rows, :] = ref[...]
        ehi[rows, :] = high
        elo[rows, :] = low
        begin += ref.shape[0]
    totals = [jnp.zeros((8, width), jnp.float32) for _ in range(2)]
    for n, (i, p) in enumerate(work):
        if n + 2 < len(work):
            copy(n + 2).start()
        copy(n).wait()
        chip = z if i < 2 else jnp.bitwise_xor(z, 1)
        j = chip * 2 + (r if i % 2 == 0 else 1 - r)
        own = pl.ds(pl.multiple_of(j * size, size), size)
        bh, bl = ehi[own, :], elo[own, :]
        for o in range(5):
            high, low = split_bf16(mbuf[n % 3, o])
            value = dot(high, bh) + dot(high, bl) + dot(low, bh)
            at = pl.ds(pl.multiple_of(lax.rem(j + o, blocks) * size, size), size)
            term = jnp.sum((e[at, :] * value).reshape(-1, 8, width), axis=0)
            totals[p] = totals[p] + (term if o in (0, 4) else 2.0 * term)
    out[...] = jnp.concatenate([jnp.sum(t, axis=0, keepdims=True) for t in totals], axis=0)


def closing_kernel(ids, weights, *refs):
    diag_out, spread_out, trial_out = refs[-3:]
    order = diag_out.shape[2]
    spread, trial = jnp.float32(0.0), jnp.float32(0.0)
    for k, ref in enumerate(refs[:-3]):
        group = jnp.bitwise_xor(ids[0], k)
        re, im = ref[0:1, :], ref[1:2, :]
        diag_out[group] = ref[0:2, :]
        spread = spread + ref[2, 0]
        trial = trial + weights[group] * jnp.sum(1.0 - re * re - im * im)
    spread_out[0] = spread
    trial_out[0] = trial / order


def lookup_weights(bvec_index, weight_table):
    table_slots = jnp.arange(weight_table.shape[0], dtype=jnp.int32)
    return jnp.sum(
        jnp.where(table_slots[None, :] == bvec_index[:, None], weight_table[None, :], 0.0), axis=1
    )


def paired(counts, m_matrices, bvec_index, weight_table, grad_prev, dir_prev):
    n_b, n_row, n_col = counts
    local_rows, local_cols = m_matrices.shape[2], m_matrices.shape[3]
    order = local_rows * n_row
    size = local_cols // n_row
    b, r, z = (lax.axis_index(a).astype(jnp.int32) for a in AXES)
    parity = jnp.bitwise_xor(b, b >> 1) & 1
    half_id = jnp.bitwise_xor(parity, z >> 1) & 1
    own_block = (z % 2) * 4 + half_id * 2 + r
    ids = jnp.stack([b, r, z, own_block, parity]).astype(jnp.int32)

    def send(x, where):
        pairs = []
        for bb in range(n_b):
            for rr in range(n_row):
                for zz in range(n_col):
                    tb, tr, tz = where(bb, rr, zz)
                    pairs.append(((bb * n_row + rr) * n_col + zz, (tb * n_row + tr) * n_col + tz))
        return lax.ppermute(x, AXES, pairs)

    core = lambda bb, rr, zz: (bb, 1 - rr, zz)
    over_b = lambda k: (lambda bb, rr, zz: (bb ^ k, rr, zz))
    over_z = lambda s: (lambda bb, rr, zz: (bb, rr, (zz + s) % n_col))
    flip_z = lambda k: (lambda bb, rr, zz: (bb, rr, zz ^ k))

    weight_all = lookup_weights(bvec_index, weight_table)
    weight_own = lax.dynamic_slice_in_dim(weight_all, b, 1)
    m = m_matrices[0]

    d_oth = send(dir_prev, core)
    packet = pl.pallas_call(
        packet_kernel, out_shape=jax.ShapeDtypeStruct((3, local_cols), jnp.float32),
        in_specs=[SMEM, ANY, ANY], out_specs=VMEM,
        scratch_shapes=[pltpu.VMEM((2, local_cols, local_cols), jnp.float32), pltpu.VMEM(grad_prev.shape, jnp.float32),
                        pltpu.SemaphoreType.DMA((3,))],
        compiler_params=pltpu.CompilerParams(vmem_limit_bytes=8 * MIB),
        cost_estimate=pl.CostEstimate(flops=10**6, bytes_accessed=1 << 22, transcendentals=0),
    )(ids, m, grad_prev)
    packet = packet + send(packet, core)
    m_oth = send(m, core)
    d_own, d_half = pl.pallas_call(
        quarter_kernel, out_shape=[jax.ShapeDtypeStruct((n, size, size), jnp.float32) for n in (4, 2)],
        in_specs=[SMEM, ANY, ANY], out_specs=[VMEM] * 2,
        scratch_shapes=[pltpu.VMEM((5, size, size), jnp.float32), pltpu.SemaphoreType.DMA((5,))],
        compiler_params=pltpu.CompilerParams(vmem_limit_bytes=8 * MIB),
        cost_estimate=pl.CostEstimate(flops=0, bytes_accessed=1 << 20, transcendentals=0),
    )(ids, dir_prev, d_oth)
    packet, d_half = lax.optimization_barrier((packet, d_half))
    diags = jnp.stack([packet] + [send(packet, over_z(s)) for s in range(1, n_col)])
    prev_square = jnp.sum(diags[:, 2, :1], axis=0)
    spread_own = weight_own[0] * jnp.sum(1.0 - diags[:, 0] ** 2 - diags[:, 1] ** 2) / order

    quarter = jax.ShapeDtypeStruct((size, size), jnp.float32)
    d_by_z = {s: send(d_half, flip_z(s)) for s in (1, 3, 2)}
    terms = pl.pallas_call(
        term_kernel, out_shape=[quarter] * 4 + [jax.ShapeDtypeStruct((2, 5, size, size), jnp.float32)],
        in_specs=[SMEM, SMEM, VMEM, ANY, ANY], out_specs=[ANY] * 5,
        scratch_shapes=[pltpu.VMEM((5, size, size), jnp.float32), pltpu.VMEM((5, size, size), jnp.float32),
                        pltpu.VMEM((4, size, size), jnp.float32),
                        pltpu.SemaphoreType.DMA((2, 5)), pltpu.SemaphoreType.DMA((4,)),
                        pltpu.SemaphoreType.DMA((2, 5))],
        compiler_params=pltpu.CompilerParams(vmem_limit_bytes=12 * MIB),
        cost_estimate=pl.CostEstimate(flops=10**9, bytes_accessed=1 << 22, transcendentals=0),
    )(ids, weight_all, diags, m, m_oth)
    parts = [send(terms[k], over_b(k)) for k in range(1, n_b)]
    g_quarter = ((terms[0] + parts[0]) + parts[1]) + parts[2]

    d_groups = [d_own] + [
        jnp.concatenate([d_by_z[s], send(d_by_z[s][:1], over_b(1)), send(d_by_z[s][1:], over_b(2))])
        for s in range(1, n_col)
    ]
    d_groups = d_groups + [send(g, core) for g in d_groups]
    g_by_z = {0: g_quarter}
    for s in (1, 3, 2):
        g_by_z[s] = send(g_quarter, flip_z(s))
    g_groups = []
    for s in range(n_col):
        piece = g_by_z[s]
        over_x = send(piece, over_b(1))
        over_y = send(piece, over_b(2))
        if s in (1, 2):
            across = send(over_y, over_b(1))
        else:
            across = send(over_x, over_b(2))
        g_groups.append(jnp.stack([piece, over_x, over_y, across]))
    g_groups = g_groups + [send(g, core) for g in g_groups]
    chosen_z = send(terms[4], flip_z(1))

    f32 = jnp.float32
    held = pltpu.VMEM((2 * n_col, 4 * size, size), f32)
    by_plane = 13 * order // 32 // 8 * 8
    shares = (by_plane, by_plane, order - 2 * by_plane)
    beta, *exp_own = pl.pallas_call(
        solve_kernel,
        out_shape=[jax.ShapeDtypeStruct((8, 128), f32)] + [jax.ShapeDtypeStruct((n, size), f32) for n in shares],
        in_specs=[SMEM, SMEM] + [ANY] * (4 * n_col), out_specs=[VMEM] * 4,
        scratch_shapes=[held, held,
                        pltpu.VMEM((order, order), jnp.bfloat16), pltpu.VMEM((order, order), jnp.bfloat16),
                        pltpu.VMEM((2, order, size), jnp.bfloat16), pltpu.VMEM((2, order, size), jnp.bfloat16),
                        pltpu.SemaphoreType.DMA((2, 2 * n_col))],
        compiler_params=pltpu.CompilerParams(vmem_limit_bytes=46 * MIB),
        cost_estimate=pl.CostEstimate(flops=7 * 3 * 2 * order * order * size, bytes_accessed=1 << 25, transcendentals=0),
    )(ids, prev_square, *g_groups, *d_groups)
    outputs = pl.pallas_call(
        output_kernel, out_shape=[jax.ShapeDtypeStruct((local_rows, local_cols), f32)] * 2,
        in_specs=[SMEM, VMEM, VMEM] + [ANY] * (2 * n_col), out_specs=[VMEM] * 2,
        scratch_shapes=[held, pltpu.SemaphoreType.DMA((2 * n_col,))],
        compiler_params=pltpu.CompilerParams(vmem_limit_bytes=VMEM_LIMIT),
        cost_estimate=pl.CostEstimate(flops=10**9, bytes_accessed=1 << 24, transcendentals=0),
    )
    grad, direction = outputs(ids, beta, dir_prev, *g_groups)

    *exp_own, chosen_z = lax.optimization_barrier((*exp_own, chosen_z))
    chosen_set = (terms[4], send(terms[4], core), chosen_z, send(chosen_z, core))
    exp_in = [send(exp_own[0], over_b(1)), send(exp_own[1], over_b(2)), send(exp_own[2], flip_z(2))]

    trial = pl.pallas_call(
        trial_kernel, out_shape=jax.ShapeDtypeStruct((2, size), f32),
        in_specs=[SMEM, VMEM, VMEM, VMEM] + [ANY] * 4, out_specs=VMEM,
        scratch_shapes=[pltpu.VMEM((order, size), f32), pltpu.VMEM((order, size), jnp.bfloat16),
                        pltpu.VMEM((order, size), jnp.bfloat16),
                        pltpu.VMEM((3, 5, size, size), f32), pltpu.SemaphoreType.DMA((3,))],
        compiler_params=pltpu.CompilerParams(vmem_limit_bytes=20 * MIB),
        cost_estimate=pl.CostEstimate(flops=3 * 2 * order * order * size, bytes_accessed=1 << 24, transcendentals=0),
    )
    t_own = trial(ids, *exp_own, *chosen_set)
    *exp_in, grad, direction = lax.optimization_barrier((*exp_in, grad, direction))
    t_in = trial(ids, *exp_in, *chosen_set)

    def ordered(bit, mine, theirs):
        return jnp.where(bit == 0, jnp.stack([mine, theirs]), jnp.stack([theirs, mine]))

    t = ordered(half_id, t_own, t_in)
    over = [send(t, flip_z(k)) for k in (2, 1, 3)]
    t = ordered(z % 2, t + over[0], over[1] + over[2])
    t = ordered(r, t, send(t, core))
    t = jnp.transpose(t, (3, 1, 2, 0, 4)).reshape(2, order)
    t = jnp.concatenate([t, jnp.full((1, order), spread_own)], axis=0)
    every = [t] + [send(t, over_b(k)) for k in range(1, n_b)]
    one = jax.ShapeDtypeStruct((1,), f32)
    trial_diag, spread, trial_spread = pl.pallas_call(
        closing_kernel, out_shape=[jax.ShapeDtypeStruct((n_b, 2, order), f32), one, one],
        in_specs=[SMEM, SMEM] + [VMEM] * n_b, out_specs=[VMEM, SMEM, SMEM],
        compiler_params=pltpu.CompilerParams(vmem_limit_bytes=4 * MIB),
    )(ids, weight_all, *every)
    return (spread.reshape(()), trial_spread.reshape(()), grad, direction, trial_diag)


def product(left, right):
    return jnp.dot(left, right, precision=HIGHEST, preferred_element_type=jnp.float32)


def shards(m_matrices, bvec_index, weight_table, grad_prev, dir_prev):
    per_group = m_matrices.shape[0]
    local_rows = m_matrices.shape[2]
    local_cols = m_matrices.shape[3]
    matrix_order = local_rows * lax.axis_size("row")
    group_index = lax.axis_index("bvec")
    row_start = lax.axis_index("row") * local_rows
    col_start = lax.axis_index("col") * local_cols
    weight_all = lookup_weights(bvec_index, weight_table)
    weight_own = lax.dynamic_slice_in_dim(weight_all, group_index * per_group, per_group)
    row_ids = row_start + jnp.arange(local_rows, dtype=jnp.int32)
    col_ids = col_start + jnp.arange(local_cols, dtype=jnp.int32)
    on_diag = (row_ids[:, None] == col_ids[None, :]).astype(jnp.float32)
    own_diag = jnp.sum(m_matrices * on_diag, axis=2)
    share_diag = lax.psum(own_diag, "row")
    diagonal = lax.all_gather(share_diag, "col", axis=2, tiled=True)
    row_diag = lax.dynamic_slice_in_dim(diagonal, row_start, local_rows, 2)
    spread_own = (
        jnp.sum(weight_own[:, None] * (1.0 - diagonal[:, 0] ** 2 - diagonal[:, 1] ** 2))
        / matrix_order
    )
    leader = (lax.axis_index("row") == 0) & (lax.axis_index("col") == 0)
    spread_term = jnp.where(leader, spread_own, 0.0)
    differ = row_diag[:, :, :, None] - share_diag[:, :, None, :]
    weighted = 2.0 * weight_own[:, None, None] * jnp.sum(m_matrices * differ, axis=1)
    grad_part = jnp.sum(weighted, axis=0)
    gradient = lax.psum(grad_part, "bvec")
    counted = jnp.where(group_index == 0, 1.0, 0.0)
    grad_square = counted * jnp.sum(gradient * gradient)
    prev_square = counted * jnp.sum(grad_prev * grad_prev)
    cross_term = counted * jnp.sum(gradient * dir_prev)
    dir_square = counted * jnp.sum(dir_prev * dir_prev)
    totals = lax.psum(
        (spread_term, grad_square, prev_square, cross_term, dir_square), ("bvec", "row", "col")
    )
    spread = totals[0]
    beta_factor = totals[1] / (1.0 + totals[2])
    direction = beta_factor * dir_prev - gradient
    dir_norm = jnp.maximum(
        totals[1] - 2.0 * beta_factor * totals[3] + beta_factor * beta_factor * totals[4], 0.0
    )
    generator = STEP_SCALE * direction / jnp.sqrt(1.0 + dir_norm / matrix_order)
    block_ids = col_start + jnp.arange(local_cols, dtype=jnp.int32)
    eye_block = (row_ids[:, None] == block_ids[None, :]).astype(jnp.float32)
    horner_start = eye_block + generator / TAYLOR
    columns = lax.all_gather(generator, "row", axis=0, tiled=True)

    def accumulate(section):
        return product(section, columns)

    def horner_step(counter, current):
        folded = accumulate(lax.all_gather(current, "col", axis=1, tiled=True))
        divisor = (TAYLOR - 1 - counter).astype(jnp.float32)
        return eye_block + folded / divisor

    expmap = lax.fori_loop(0, TAYLOR - 1, horner_step, horner_start)
    expmap_cols = lax.all_gather(expmap, "row", axis=0, tiled=True)
    section = lax.all_gather(m_matrices, "col", axis=3, tiled=True)
    flattened = section.reshape((-1, section.shape[3]))
    rotated = product(flattened, expmap_cols).reshape(
        jnp.zeros(m_matrices.shape, jnp.float32).shape
    )
    trial_part = jnp.sum(expmap[None, None] * rotated, axis=2)
    trial_share = lax.psum(trial_part, "row")
    trial_group = lax.all_gather(trial_share, "col", axis=2, tiled=True)
    trial_diag = lax.all_gather(trial_group, "bvec", axis=0, tiled=True)
    trial_spread = (
        jnp.sum(weight_all[:, None] * (1.0 - trial_diag[:, 0] ** 2 - trial_diag[:, 1] ** 2))
        / matrix_order
    )
    return (spread, trial_spread, gradient, direction, trial_diag)


def solution(mesh):
    placed = (P("bvec", None, "row", "col"), P(), P(), P("row", "col"), P("row", "col"))
    counts = tuple(mesh.shape[a] for a in AXES)
    special = counts == (4, 2, 4)

    def named(*args):
        return paired(counts, *args)

    return jax.shard_map(
        named if special else shards,
        mesh=mesh,
        in_specs=placed,
        out_specs=(P(), P(), P("row", "col"), P("row", "col"), P()),
        check_vma=False,
    )
```

```python
import jax
import jax.numpy as jnp
from jax import lax
from jax.experimental import pallas as pl
from jax.experimental.pallas import tpu as pltpu
from jax.sharding import PartitionSpec as P


TAYLOR = 8
STEP_SCALE = 1.75
HIGHEST = lax.Precision.HIGHEST
AXES = ("bvec", "row", "col")
ANY = pl.BlockSpec(memory_space=pl.ANY)
SMEM = pl.BlockSpec(memory_space=pltpu.SMEM)
VMEM = pl.BlockSpec(memory_space=pltpu.VMEM)
MIB = 1024 * 1024
VMEM_LIMIT = 62 * MIB


def split_bf16(x):
    high = x.astype(jnp.bfloat16)
    low = (x - high.astype(jnp.float32)).astype(jnp.bfloat16)
    return high, low


def dot(a, b):
    return jnp.dot(a, b, preferred_element_type=jnp.float32)


def above(n):
    return lax.broadcasted_iota(jnp.int32, (n, n), 1) > lax.broadcasted_iota(jnp.int32, (n, n), 0)


def pack_block(part, o, value, low_half):
    n = value.shape[0] // 2

    def put(i, rows):
        part[i // 2, i % 2 * n:(i % 2 + 1) * n, :] = rows

    if o == 0:
        mixed = jnp.where(above(n), value[:n, :n], value[n:, n:])
        put(0, jnp.concatenate([mixed, value[:n, n:]], axis=1))
    elif o == 4:
        put(7, jnp.where(low_half, value[:n, :], value[:, n:].T))
    else:
        put(2 * o - 1, value[:n])
        put(2 * o, value[n:])


def unpack_diagonal(rows):
    n = rows.shape[0]
    mixed, corner = rows[:, :n], rows[:, n:]
    upper = jnp.where(above(n), mixed, 0.0)
    below = lax.broadcasted_iota(jnp.int32, (n, n), 1) < lax.broadcasted_iota(jnp.int32, (n, n), 0)
    lower = jnp.where(below, mixed, 0.0)
    return upper - upper.T, corner, -corner.T, lower - lower.T


def packet_kernel(ids, m, prev, out, square, gprev, sem):
    r, z = ids[1], ids[2]
    n = square.shape[1]
    per_core = m.shape[1] // n
    rows = pl.ds(pl.multiple_of(lax.rem(z, per_core) * n, n), n)
    squares = [pltpu.make_async_copy(m.at[p, rows, :], square.at[p], sem.at[p]) for p in range(2)]
    other = pltpu.make_async_copy(prev, gprev, sem.at[2])
    holder = lax.div(z, per_core) == r
    other.start()

    @pl.when(holder)
    def _():
        for c in squares:
            c.start()
        on_diag = lax.broadcasted_iota(jnp.int32, (n, n), 0) == lax.broadcasted_iota(jnp.int32, (n, n), 1)
        for p, c in enumerate(squares):
            c.wait()
            out[p:p + 1, :] = jnp.sum(jnp.where(on_diag, square[p], 0.0), axis=0, keepdims=True)

    @pl.when(jnp.logical_not(holder))
    def _():
        out[0:2, :] = jnp.zeros((2, n), jnp.float32)

    other.wait()
    g = gprev[...]
    total = jnp.sum(jnp.sum((g * g).reshape(-1, 8, n), axis=0))
    out[2:3, :] = jnp.full((1, n), total, jnp.float32)


def term_kernel(ids, weight, diags, own, other, o0, o1, o2, o3, chosen, mre, mim, part, sem, out_sem, chosen_sem):
    b, r, z = ids[0], ids[1], ids[2]
    size = mre.shape[-1]
    per_core = own.shape[1] // size
    blocks = 2 * per_core
    kept = mre.shape[0]
    per_chip = own.shape[2] // size
    groups = blocks // per_chip
    j = z * per_chip + r
    lanes = pl.ds(pl.multiple_of(r * size, size), size)
    for o in range(kept):
        block = lax.rem(j + o, blocks)
        rows = pl.ds(pl.multiple_of(lax.rem(block, per_core) * size, size), size)
        mine = lax.div(block, per_core) == r
        for ref, cond in ((own, mine), (other, jnp.logical_not(mine))):
            @pl.when(cond)
            def _(ref=ref, o=o, rows=rows):
                pltpu.make_async_copy(ref.at[0, rows, lanes], mre.at[o], sem.at[0, o]).start()
                pltpu.make_async_copy(ref.at[1, rows, lanes], mim.at[o], sem.at[1, o]).start()

    def piece(block, p):
        slot = lax.rem(z - lax.div(block, per_chip) + groups, groups)
        half = lax.rem(block, per_chip)
        row = diags[slot, pl.ds(p, 1), :]
        return jnp.where(half == 0, row[:, :size], row[:, size:])

    factor = 2.0 * weight[b]
    re_own, im_own = piece(j, 0), piece(j, 1)
    low_half = j < blocks // 2
    copies = []
    for o in range(kept):
        block = lax.rem(j + o, blocks)
        re_rows = jnp.broadcast_to(piece(block, 0), (size, size)).T
        im_rows = jnp.broadcast_to(piece(block, 1), (size, size)).T
        pltpu.make_async_copy(own.at[0, pl.ds(0, size), pl.ds(0, size)], mre.at[o], sem.at[0, o]).wait()
        pltpu.make_async_copy(own.at[0, pl.ds(0, size), pl.ds(0, size)], mim.at[o], sem.at[1, o]).wait()
        kept_copies = [pltpu.make_async_copy(buf.at[o], chosen.at[p, o], chosen_sem.at[p, o]) for p, buf in enumerate((mre, mim))]
        for copy in kept_copies:
            copy.start()
        copies += kept_copies
        value = factor * (mre[o] * (re_rows - re_own) + mim[o] * (im_rows - im_own))
        pack_block(part, o, value, low_half)
    for k, out in enumerate((o0, o1, o2, o3)):
        copy = pltpu.make_async_copy(part.at[jnp.bitwise_xor(b, k)], out, out_sem.at[k])
        copy.start()
        copies.append(copy)
    for copy in copies:
        copy.wait()


def quarter_kernel(ids, own, other, out, half, buf, sem):
    r, z, h = ids[1], ids[2], ids[4]
    size = buf.shape[2]
    per_core = own.shape[0] // size
    blocks = 2 * per_core
    per_chip = own.shape[1] // size
    j = z * per_chip + r
    lanes = pl.ds(pl.multiple_of(r * size, size), size)
    for o in range(5):
        block = lax.rem(j + o, blocks)
        rows = pl.ds(pl.multiple_of(lax.rem(block, per_core) * size, size), size)
        mine = lax.div(block, per_core) == r
        for ref, cond in ((own, mine), (other, jnp.logical_not(mine))):
            @pl.when(cond)
            def _(ref=ref, rows=rows, o=o):
                pltpu.make_async_copy(ref.at[rows, lanes], buf.at[o], sem.at[o]).start()
    for o in range(5):
        pltpu.make_async_copy(own.at[pl.ds(0, size), pl.ds(0, size)], buf.at[o], sem.at[o]).wait()
        pack_block(out, o, buf[o], j < blocks // 2)
    half[...] = jnp.where(h == 0, out[0:2], out[2:4])


def group_copies(ids, ins, dst, sem, place):
    r, z = ids[1], ids[2]
    groups = len(ins) // 2
    quarter = ins[0].shape[1]
    out = []
    for i, ref in enumerate(ins):
        s, c = i % groups, i // groups
        j = jnp.bitwise_xor(z, s) * 2 + (r if c == 0 else 1 - r)
        for k in range(4):
            rows = pl.ds(pl.multiple_of(place(s, k) * quarter, quarter), quarter)
            out.append(pltpu.make_async_copy(ref.at[k], dst.at[j, rows], sem.at[i]))
    return out


def terms_place(ids):
    return lambda s, k: jnp.bitwise_xor(ids[0], k)


def shared_place(ids):
    h = ids[4]
    return lambda s, k: k if s == 0 else (2 * h + k if k < 2 else 2 * (1 - h) + k - 2)


def solve_kernel(ids, prev_square, *refs):
    groups = (len(refs) - 11) // 4
    g_in, d_in = refs[:2 * groups], refs[2 * groups:4 * groups]
    beta_out, exp_a, exp_b, exp_c, pg, pd, ahi, alo, hhi, hlo, sem = refs[4 * groups:]
    own_block = ids[3]
    order = ahi.shape[0]
    blocks, _, size = pg.shape

    g_copies = group_copies(ids, g_in, pg, sem.at[0], terms_place(ids))
    d_copies = group_copies(ids, d_in, pd, sem.at[1], shared_place(ids))
    for c in g_copies + d_copies:
        c.start()
    strip = size // 2

    def fold(x):
        return jnp.sum(x.reshape(-1, 8, size), axis=0)

    quarter = g_in[0].shape[1]

    def arrive(which, i):
        for k in range(4):
            at = pl.ds(k * quarter, quarter)
            pltpu.make_async_copy(g_in[0].at[k], pg.at[0, at], sem.at[which, i]).wait()
        core = lax.div(i, groups)
        column = jnp.bitwise_xor(ids[2], lax.rem(i, groups)) * 2
        return column + jnp.where(core == 0, ids[1], 1 - ids[1])

    def norm_body(i, acc):
        jj = arrive(0, i)
        for t in range(0, pg.shape[1], size):
            v = pg[jj, t:t + size, :]
            acc = acc + fold(v * v)
        return acc

    zero = jnp.zeros((8, size), jnp.float32)
    beta = 2.0 * jnp.sum(lax.fori_loop(0, blocks, norm_body, zero)) / (1.0 + prev_square[0])
    beta_out[...] = jnp.full(beta_out.shape, beta, jnp.float32)

    def store(row, col, v):
        high, low = split_bf16(v)
        rows = pl.ds(pl.multiple_of(row, strip), v.shape[0])
        cols = pl.ds(pl.multiple_of(col, strip), v.shape[1])
        ahi[rows, cols] = high
        alo[rows, cols] = low

    def dir_body(i, acc):
        jj = arrive(1, i)
        base = jj * size
        for t in range(8):
            at = slice(t * strip, (t + 1) * strip)
            v = beta * pd[jj, at, :] - pg[jj, at, :]
            acc = acc + fold(v * v)
            if t == 0:
                first_q, second_q, third_q, fourth_q = unpack_diagonal(v)
                store(base, base, first_q)
                store(base, base + strip, second_q)
                store(base + strip, base, third_q)
                store(base + strip, base + strip, fourth_q)
            elif t == 7:
                low_half = jj < blocks // 2
                v = jnp.where(low_half, v, -v)
                high_block = jnp.where(low_half, jj + blocks // 2, jj) * size + jnp.where(low_half, 0, strip)
                low_block = jnp.where(low_half, jj, jj - blocks // 2) * size
                store(high_block, low_block, v)
                store(low_block, high_block, -v.T)
            else:
                row = lax.rem(jj + (t + 1) // 2, blocks) * size + (t + 1) % 2 * strip
                store(row, base, v)
                store(base, row, -v.T)
        return acc

    dir_square = 2.0 * jnp.sum(lax.fori_loop(0, blocks, dir_body, zero))
    scale = STEP_SCALE / jnp.sqrt(jnp.full((1, size), 1.0 + dir_square / order, jnp.float32))

    tile = min(1024, order)
    own_cols = pl.ds(pl.multiple_of(own_block * size, size), size)

    def eye_rows(start, count):
        rid = lax.broadcasted_iota(jnp.int32, (count, size), 0) + start
        cid = lax.broadcasted_iota(jnp.int32, (count, size), 1) + own_block * size
        return (rid == cid).astype(jnp.float32)

    def first(i, carry):
        start = pl.multiple_of(i * size, size)
        rows = pl.ds(start, size)
        a = ahi[rows, own_cols].astype(jnp.float32) + alo[rows, own_cols].astype(jnp.float32)
        high, low = split_bf16(eye_rows(start, size) + a * (scale / TAYLOR))
        hhi[0, rows, :] = high
        hlo[0, rows, :] = low
        return carry

    lax.fori_loop(0, order // size, first, 0)

    def step(counter, carry):
        now = lax.rem(counter, 2)
        divisor = (TAYLOR - 1 - counter).astype(jnp.float32)
        inverse = scale / jnp.full((1, size), divisor, jnp.float32)
        bh = hhi[now]
        bl = hlo[now]

        def rows_body(i, c):
            start = pl.multiple_of(i * tile, tile)
            rows = pl.ds(start, tile)
            ah, al = ahi[rows, :], alo[rows, :]
            value = eye_rows(start, tile) + (dot(ah, bh) + dot(ah, bl) + dot(al, bh)) * inverse

            @pl.when(counter < TAYLOR - 2)
            def _():
                high, low = split_bf16(value)
                hhi[1 - now, rows, :] = high
                hlo[1 - now, rows, :] = low

            for t in range(order // tile):
                @pl.when((counter == TAYLOR - 2) & (i == t))
                def _(t=t):
                    begin = 0
                    for ref in (exp_a, exp_b, exp_c):
                        end = begin + ref.shape[0]
                        lo, hi = max(begin, t * tile), min(end, (t + 1) * tile)
                        if lo < hi:
                            ref[lo - begin:hi - begin, :] = value[lo - t * tile:hi - t * tile]
                        begin = end
            return c

        return lax.fori_loop(0, order // tile, rows_body, carry)

    lax.fori_loop(0, TAYLOR - 1, step, 0)


def output_kernel(ids, beta, dprev, *refs):
    g_in = refs[:-8]
    grad_to, dir_to, pg, prev, grad_out, dir_out, sem, out_sem = refs[-8:]
    r, z = ids[1], ids[2]
    blocks, _, size = pg.shape
    per_core = grad_out.shape[0] // size
    per_chip = grad_out.shape[1] // size
    groups = len(g_in) // 2
    prev_copy = pltpu.make_async_copy(dprev, prev, out_sem.at[2, 0])
    copies = group_copies(ids, g_in, pg, sem, terms_place(ids))

    def needed(n):
        return jnp.bitwise_xor(z, n // 4 % groups) != lax.rem(z + 1, groups)

    for n, c in enumerate(copies):
        pl.when(needed(n))(c.start)
    prev_copy.start()
    for n, c in enumerate(copies):
        pl.when(needed(n))(c.wait)
    prev_copy.wait()

    def out_body(t, carry):
        i, jx = lax.div(t, per_chip), lax.rem(t, per_chip)
        rb, cb = r * per_core + i, z * per_chip + jx
        o = lax.rem(rb - cb + blocks, blocks)
        rows = pl.ds(pl.multiple_of(i * size, size), size)
        cols = pl.ds(pl.multiple_of(jx * size, size), size)

        n = size // 2

        @pl.when(o == 0)
        def _():
            first_q, second_q, third_q, fourth_q = unpack_diagonal(pg[cb, :n, :])
            grad_out[rows, cols] = jnp.concatenate(
                [jnp.concatenate([first_q, second_q], axis=1), jnp.concatenate([third_q, fourth_q], axis=1)], axis=0)

        @pl.when((o > 0) & (o < 4))
        def _():
            grad_out[rows, cols] = pg[cb, pl.ds(pl.multiple_of(o * size - n, n), size), :]

        @pl.when(o > 4)
        def _():
            grad_out[rows, cols] = -pg[rb, pl.ds(pl.multiple_of((blocks - o) * size - n, n), size), :].T

        @pl.when((o == 4) & (rb > cb))
        def _():
            grad_out[rows, cols] = jnp.concatenate([pg[cb, 7 * n:, :], -pg[rb, 7 * n:, :]], axis=0)

        @pl.when((o == 4) & (rb < cb))
        def _():
            grad_out[rows, cols] = jnp.concatenate([-pg[rb, 7 * n:, :], pg[cb, 7 * n:, :]], axis=0).T

        dir_out[rows, cols] = beta[0:1, 0:1] * prev[rows, cols] - grad_out[rows, cols]
        pltpu.make_async_copy(grad_out.at[rows, cols], grad_to.at[rows, cols], out_sem.at[0, t]).start()
        pltpu.make_async_copy(dir_out.at[rows, cols], dir_to.at[rows, cols], out_sem.at[1, t]).start()
        return carry

    count = per_core * per_chip
    lax.fori_loop(0, count, out_body, 0)
    for t in range(count):
        rows = pl.ds(t // per_chip * size, size)
        cols = pl.ds(t % per_chip * size, size)
        pltpu.make_async_copy(grad_out.at[rows, cols], grad_to.at[rows, cols], out_sem.at[0, t]).wait()
        pltpu.make_async_copy(dir_out.at[rows, cols], dir_to.at[rows, cols], out_sem.at[1, t]).wait()


def trial_kernel(ids, exp_a, exp_b, exp_c, m0, m1, m2, m3, out, e, ehi, elo, mbuf, sem):
    r, z = ids[1], ids[2]
    width = exp_a.shape[1]
    size = m0.shape[2]
    blocks = e.shape[0] // size
    work = [(i, p) for i in range(4) for p in range(2)]
    sources = (m0, m1, m2, m3)

    def copy(n):
        i, p = work[n]
        return pltpu.make_async_copy(sources[i].at[p], mbuf.at[n % 3], sem.at[n % 3])

    copy(0).start()
    copy(1).start()
    begin = 0
    for ref in (exp_a, exp_b, exp_c):
        high, low = split_bf16(ref[...])
        rows = slice(begin, begin + ref.shape[0])
        e[rows, :] = ref[...]
        ehi[rows, :] = high
        elo[rows, :] = low
        begin += ref.shape[0]
    totals = [jnp.zeros((8, width), jnp.float32) for _ in range(2)]
    for n, (i, p) in enumerate(work):
        if n + 2 < len(work):
            copy(n + 2).start()
        copy(n).wait()
        chip = z if i < 2 else jnp.bitwise_xor(z, 1)
        j = chip * 2 + (r if i % 2 == 0 else 1 - r)
        own = pl.ds(pl.multiple_of(j * size, size), size)
        bh, bl = ehi[own, :], elo[own, :]
        for o in range(5):
            high, low = split_bf16(mbuf[n % 3, o])
            value = dot(high, bh) + dot(high, bl) + dot(low, bh)
            at = pl.ds(pl.multiple_of(lax.rem(j + o, blocks) * size, size), size)
            term = jnp.sum((e[at, :] * value).reshape(-1, 8, width), axis=0)
            totals[p] = totals[p] + (term if o in (0, 4) else 2.0 * term)
    out[...] = jnp.concatenate([jnp.sum(t, axis=0, keepdims=True) for t in totals], axis=0)


def closing_kernel(ids, weights, *refs):
    diag_out, spread_out, trial_out = refs[-3:]
    order = diag_out.shape[2]
    spread, trial = jnp.float32(0.0), jnp.float32(0.0)
    for k, ref in enumerate(refs[:-3]):
        group = jnp.bitwise_xor(ids[0], k)
        re, im = ref[0:1, :], ref[1:2, :]
        diag_out[group] = ref[0:2, :]
        spread = spread + ref[2, 0]
        trial = trial + weights[group] * jnp.sum(1.0 - re * re - im * im)
    spread_out[0] = spread
    trial_out[0] = trial / order


def lookup_weights(bvec_index, weight_table):
    table_slots = jnp.arange(weight_table.shape[0], dtype=jnp.int32)
    return jnp.sum(
        jnp.where(table_slots[None, :] == bvec_index[:, None], weight_table[None, :], 0.0), axis=1
    )


def paired(counts, m_matrices, bvec_index, weight_table, grad_prev, dir_prev):
    n_b, n_row, n_col = counts
    local_rows, local_cols = m_matrices.shape[2], m_matrices.shape[3]
    order = local_rows * n_row
    size = local_cols // n_row
    b, r, z = (lax.axis_index(a).astype(jnp.int32) for a in AXES)
    parity = jnp.bitwise_xor(b, b >> 1) & 1
    half_id = jnp.bitwise_xor(parity, z >> 1) & 1
    own_block = (z % 2) * 4 + half_id * 2 + r
    ids = jnp.stack([b, r, z, own_block, parity]).astype(jnp.int32)

    def send(x, where):
        pairs = []
        for bb in range(n_b):
            for rr in range(n_row):
                for zz in range(n_col):
                    tb, tr, tz = where(bb, rr, zz)
                    pairs.append(((bb * n_row + rr) * n_col + zz, (tb * n_row + tr) * n_col + tz))
        return lax.ppermute(x, AXES, pairs)

    core = lambda bb, rr, zz: (bb, 1 - rr, zz)
    over_b = lambda k: (lambda bb, rr, zz: (bb ^ k, rr, zz))
    over_z = lambda s: (lambda bb, rr, zz: (bb, rr, (zz + s) % n_col))
    flip_z = lambda k: (lambda bb, rr, zz: (bb, rr, zz ^ k))

    weight_all = lookup_weights(bvec_index, weight_table)
    weight_own = lax.dynamic_slice_in_dim(weight_all, b, 1)
    m = m_matrices[0]

    d_oth = send(dir_prev, core)
    packet = pl.pallas_call(
        packet_kernel, out_shape=jax.ShapeDtypeStruct((3, local_cols), jnp.float32),
        in_specs=[SMEM, ANY, ANY], out_specs=VMEM,
        scratch_shapes=[pltpu.VMEM((2, local_cols, local_cols), jnp.float32), pltpu.VMEM(grad_prev.shape, jnp.float32),
                        pltpu.SemaphoreType.DMA((3,))],
        compiler_params=pltpu.CompilerParams(vmem_limit_bytes=8 * MIB),
        cost_estimate=pl.CostEstimate(flops=10**6, bytes_accessed=1 << 22, transcendentals=0),
    )(ids, m, grad_prev)
    packet = packet + send(packet, core)
    m_oth = send(m, core)
    d_own, d_half = pl.pallas_call(
        quarter_kernel, out_shape=[jax.ShapeDtypeStruct((n, size, size), jnp.float32) for n in (4, 2)],
        in_specs=[SMEM, ANY, ANY], out_specs=[VMEM] * 2,
        scratch_shapes=[pltpu.VMEM((5, size, size), jnp.float32), pltpu.SemaphoreType.DMA((5,))],
        compiler_params=pltpu.CompilerParams(vmem_limit_bytes=8 * MIB),
        cost_estimate=pl.CostEstimate(flops=0, bytes_accessed=1 << 20, transcendentals=0),
    )(ids, dir_prev, d_oth)
    packet, d_half = lax.optimization_barrier((packet, d_half))
    diags = jnp.stack([packet] + [send(packet, over_z(s)) for s in range(1, n_col)])
    prev_square = jnp.sum(diags[:, 2, :1], axis=0)
    spread_own = weight_own[0] * jnp.sum(1.0 - diags[:, 0] ** 2 - diags[:, 1] ** 2) / order

    quarter = jax.ShapeDtypeStruct((size, size), jnp.float32)
    d_by_z = {s: send(d_half, flip_z(s)) for s in (1, 3, 2)}
    terms = pl.pallas_call(
        term_kernel, out_shape=[quarter] * 4 + [jax.ShapeDtypeStruct((2, 5, size, size), jnp.float32)],
        in_specs=[SMEM, SMEM, VMEM, ANY, ANY], out_specs=[ANY] * 5,
        scratch_shapes=[pltpu.VMEM((5, size, size), jnp.float32), pltpu.VMEM((5, size, size), jnp.float32),
                        pltpu.VMEM((4, size, size), jnp.float32),
                        pltpu.SemaphoreType.DMA((2, 5)), pltpu.SemaphoreType.DMA((4,)),
                        pltpu.SemaphoreType.DMA((2, 5))],
        compiler_params=pltpu.CompilerParams(vmem_limit_bytes=12 * MIB),
        cost_estimate=pl.CostEstimate(flops=10**9, bytes_accessed=1 << 22, transcendentals=0),
    )(ids, weight_all, diags, m, m_oth)
    parts = [send(terms[k], over_b(k)) for k in range(1, n_b)]
    g_quarter = ((terms[0] + parts[0]) + parts[1]) + parts[2]

    d_groups = [d_own] + [
        jnp.concatenate([d_by_z[s], send(d_by_z[s][:1], over_b(1)), send(d_by_z[s][1:], over_b(2))])
        for s in range(1, n_col)
    ]
    d_groups = d_groups + [send(g, core) for g in d_groups]
    g_by_z = {0: g_quarter}
    for s in (1, 3, 2):
        g_by_z[s] = send(g_quarter, flip_z(s))
    g_groups = []
    for s in range(n_col):
        piece = g_by_z[s]
        over_x = send(piece, over_b(1))
        over_y = send(piece, over_b(2))
        if s in (1, 2):
            across = send(over_y, over_b(1))
        else:
            across = send(over_x, over_b(2))
        g_groups.append(jnp.stack([piece, over_x, over_y, across]))
    g_groups = g_groups + [send(g, core) for g in g_groups]
    chosen_z = send(terms[4], flip_z(1))

    f32 = jnp.float32
    held = pltpu.VMEM((2 * n_col, 4 * size, size), f32)
    by_plane = 27 * order // 64 // 8 * 8
    shares = (by_plane, by_plane, order - 2 * by_plane)
    beta, *exp_own = pl.pallas_call(
        solve_kernel,
        out_shape=[jax.ShapeDtypeStruct((8, 128), f32)] + [jax.ShapeDtypeStruct((n, size), f32) for n in shares],
        in_specs=[SMEM, SMEM] + [ANY] * (4 * n_col), out_specs=[VMEM] * 4,
        scratch_shapes=[held, held,
                        pltpu.VMEM((order, order), jnp.bfloat16), pltpu.VMEM((order, order), jnp.bfloat16),
                        pltpu.VMEM((2, order, size), jnp.bfloat16), pltpu.VMEM((2, order, size), jnp.bfloat16),
                        pltpu.SemaphoreType.DMA((2, 2 * n_col))],
        compiler_params=pltpu.CompilerParams(vmem_limit_bytes=46 * MIB),
        cost_estimate=pl.CostEstimate(flops=7 * 3 * 2 * order * order * size, bytes_accessed=1 << 25, transcendentals=0),
    )(ids, prev_square, *g_groups, *d_groups)
    outputs = pl.pallas_call(
        output_kernel, out_shape=[jax.ShapeDtypeStruct((local_rows, local_cols), f32)] * 2,
        in_specs=[SMEM, VMEM, ANY] + [ANY] * (2 * n_col), out_specs=[ANY] * 2,
        scratch_shapes=[held] + [pltpu.VMEM((local_rows, local_cols), f32)] * 3 + [
            pltpu.SemaphoreType.DMA((2 * n_col,)), pltpu.SemaphoreType.DMA((3, 2 * n_col))],
        compiler_params=pltpu.CompilerParams(vmem_limit_bytes=VMEM_LIMIT),
        cost_estimate=pl.CostEstimate(flops=10**9, bytes_accessed=1 << 24, transcendentals=0),
    )
    grad, direction = outputs(ids, beta, dir_prev, *g_groups)

    *exp_own, chosen_z = lax.optimization_barrier((*exp_own, chosen_z))
    chosen_set = (terms[4], send(terms[4], core), chosen_z, send(chosen_z, core))
    exp_in = [send(exp_own[0], over_b(1)), send(exp_own[1], over_b(2)), send(exp_own[2], flip_z(2))]

    trial = pl.pallas_call(
        trial_kernel, out_shape=jax.ShapeDtypeStruct((2, size), f32),
        in_specs=[SMEM, VMEM, VMEM, VMEM] + [ANY] * 4, out_specs=VMEM,
        scratch_shapes=[pltpu.VMEM((order, size), f32), pltpu.VMEM((order, size), jnp.bfloat16),
                        pltpu.VMEM((order, size), jnp.bfloat16),
                        pltpu.VMEM((3, 5, size, size), f32), pltpu.SemaphoreType.DMA((3,))],
        compiler_params=pltpu.CompilerParams(vmem_limit_bytes=20 * MIB),
        cost_estimate=pl.CostEstimate(flops=3 * 2 * order * order * size, bytes_accessed=1 << 24, transcendentals=0),
    )
    t_own = trial(ids, *exp_own, *chosen_set)
    *exp_in, grad, direction = lax.optimization_barrier((*exp_in, grad, direction))
    t_in = trial(ids, *exp_in, *chosen_set)

    def ordered(bit, mine, theirs):
        return jnp.where(bit == 0, jnp.stack([mine, theirs]), jnp.stack([theirs, mine]))

    t = ordered(half_id, t_own, t_in)
    over = [send(t, flip_z(k)) for k in (2, 1, 3)]
    t = ordered(z % 2, t + over[0], over[1] + over[2])
    t = ordered(r, t, send(t, core))
    t = jnp.transpose(t, (3, 1, 2, 0, 4)).reshape(2, order)
    t = jnp.concatenate([t, jnp.full((1, order), spread_own)], axis=0)
    every = [t] + [send(t, over_b(k)) for k in range(1, n_b)]
    one = jax.ShapeDtypeStruct((1,), f32)
    trial_diag, spread, trial_spread = pl.pallas_call(
        closing_kernel, out_shape=[jax.ShapeDtypeStruct((n_b, 2, order), f32), one, one],
        in_specs=[SMEM, SMEM] + [VMEM] * n_b, out_specs=[VMEM, SMEM, SMEM],
        compiler_params=pltpu.CompilerParams(vmem_limit_bytes=4 * MIB),
    )(ids, weight_all, *every)
    return (spread.reshape(()), trial_spread.reshape(()), grad, direction, trial_diag)


def product(left, right):
    return jnp.dot(left, right, precision=HIGHEST, preferred_element_type=jnp.float32)


def shards(m_matrices, bvec_index, weight_table, grad_prev, dir_prev):
    per_group = m_matrices.shape[0]
    local_rows = m_matrices.shape[2]
    local_cols = m_matrices.shape[3]
    matrix_order = local_rows * lax.axis_size("row")
    group_index = lax.axis_index("bvec")
    row_start = lax.axis_index("row") * local_rows
    col_start = lax.axis_index("col") * local_cols
    weight_all = lookup_weights(bvec_index, weight_table)
    weight_own = lax.dynamic_slice_in_dim(weight_all, group_index * per_group, per_group)
    row_ids = row_start + jnp.arange(local_rows, dtype=jnp.int32)
    col_ids = col_start + jnp.arange(local_cols, dtype=jnp.int32)
    on_diag = (row_ids[:, None] == col_ids[None, :]).astype(jnp.float32)
    own_diag = jnp.sum(m_matrices * on_diag, axis=2)
    share_diag = lax.psum(own_diag, "row")
    diagonal = lax.all_gather(share_diag, "col", axis=2, tiled=True)
    row_diag = lax.dynamic_slice_in_dim(diagonal, row_start, local_rows, 2)
    spread_own = (
        jnp.sum(weight_own[:, None] * (1.0 - diagonal[:, 0] ** 2 - diagonal[:, 1] ** 2))
        / matrix_order
    )
    leader = (lax.axis_index("row") == 0) & (lax.axis_index("col") == 0)
    spread_term = jnp.where(leader, spread_own, 0.0)
    differ = row_diag[:, :, :, None] - share_diag[:, :, None, :]
    weighted = 2.0 * weight_own[:, None, None] * jnp.sum(m_matrices * differ, axis=1)
    grad_part = jnp.sum(weighted, axis=0)
    gradient = lax.psum(grad_part, "bvec")
    counted = jnp.where(group_index == 0, 1.0, 0.0)
    grad_square = counted * jnp.sum(gradient * gradient)
    prev_square = counted * jnp.sum(grad_prev * grad_prev)
    cross_term = counted * jnp.sum(gradient * dir_prev)
    dir_square = counted * jnp.sum(dir_prev * dir_prev)
    totals = lax.psum(
        (spread_term, grad_square, prev_square, cross_term, dir_square), ("bvec", "row", "col")
    )
    spread = totals[0]
    beta_factor = totals[1] / (1.0 + totals[2])
    direction = beta_factor * dir_prev - gradient
    dir_norm = jnp.maximum(
        totals[1] - 2.0 * beta_factor * totals[3] + beta_factor * beta_factor * totals[4], 0.0
    )
    generator = STEP_SCALE * direction / jnp.sqrt(1.0 + dir_norm / matrix_order)
    block_ids = col_start + jnp.arange(local_cols, dtype=jnp.int32)
    eye_block = (row_ids[:, None] == block_ids[None, :]).astype(jnp.float32)
    horner_start = eye_block + generator / TAYLOR
    columns = lax.all_gather(generator, "row", axis=0, tiled=True)

    def accumulate(section):
        return product(section, columns)

    def horner_step(counter, current):
        folded = accumulate(lax.all_gather(current, "col", axis=1, tiled=True))
        divisor = (TAYLOR - 1 - counter).astype(jnp.float32)
        return eye_block + folded / divisor

    expmap = lax.fori_loop(0, TAYLOR - 1, horner_step, horner_start)
    expmap_cols = lax.all_gather(expmap, "row", axis=0, tiled=True)
    section = lax.all_gather(m_matrices, "col", axis=3, tiled=True)
    flattened = section.reshape((-1, section.shape[3]))
    rotated = product(flattened, expmap_cols).reshape(
        jnp.zeros(m_matrices.shape, jnp.float32).shape
    )
    trial_part = jnp.sum(expmap[None, None] * rotated, axis=2)
    trial_share = lax.psum(trial_part, "row")
    trial_group = lax.all_gather(trial_share, "col", axis=2, tiled=True)
    trial_diag = lax.all_gather(trial_group, "bvec", axis=0, tiled=True)
    trial_spread = (
        jnp.sum(weight_all[:, None] * (1.0 - trial_diag[:, 0] ** 2 - trial_diag[:, 1] ** 2))
        / matrix_order
    )
    return (spread, trial_spread, gradient, direction, trial_diag)


def solution(mesh):
    placed = (P("bvec", None, "row", "col"), P(), P(), P("row", "col"), P("row", "col"))
    counts = tuple(mesh.shape[a] for a in AXES)
    special = counts == (4, 2, 4)

    def named(*args):
        return paired(counts, *args)

    return jax.shard_map(
        named if special else shards,
        mesh=mesh,
        in_specs=placed,
        out_specs=(P(), P(), P("row", "col"), P("row", "col"), P()),
        check_vma=False,
    )
```
